32 devices in a mesh: wav: 8 (over y, x, core), lev: 4 (over z).
Axes of the slice: x: 2, y: 2, z: 4, core: 2. Of those that a mesh axis runs over, the one named last changes fastest.
Arguments:
- spectral: bfloat16 [200, 401, 512], P('wav', None, 'lev'), may hold values from -0.1796875 to 0.1796875
- legendre: bfloat16 [200, 401, 64], P('wav', None, 'lev'), may hold values from -0.4375 to 0.4375
- wave_pair: int32 [200], replicated, may hold values from -1 to 199, as said below
- lat_slot: int32 [64], replicated, may hold values from 0 to 799, as said below
Outputs:
- gridded: bfloat16 [64, 256, 1616], P('wav', 'lev')
The draws below stay inside these ranges and needn't reach their ends.
Inputs may be any that keep to these rules, and one draw needn't show every extreme that they name: `wave_pair`: each pair number 0 to 199 appears exactly once; all other entries are -1. `lat_slot`: the entries are distinct latitudes.
All inputs are finite; a program needn't handle non-finite values.
Results may differ from the reference program's by a relative error of at most 0.0055.
Values may be sent and summed in bfloat16 or wider, within the bound.
A program may use at most 64 MiB of HBM per device.

```python
import math
import jax
import jax.numpy as jnp
from jax import lax

WAVES = 400
NLAT = 800
PAIRS = 200
FOLD = 401
WSLOTS = 200
NROWS = 64
LAYERS = 256


def draw_wave_pair(key, part):
    order = jax.random.permutation(jax.random.fold_in(key, 11), WSLOTS)
    return jnp.where(order < PAIRS, order, -1).astype(jnp.int32)


def draw_lat_slot(key, part):
    order = jax.random.permutation(jax.random.fold_in(key, 13), NLAT)
    return order[:NROWS].astype(jnp.int32)


def levels(own_key, extent, shards, least, high):
    gain = 1.0
    for dim, parts in shards:
        heights = jax.random.uniform(jax.random.fold_in(jax.random.fold_in(own_key, 6), dim), (parts,), jnp.float32, least / len(shards), high / len(shards))
        gain = gain * jnp.repeat(jnp.exp(heights), extent[dim] // parts).reshape((-1,) + (1,) * (len(extent) - 1 - dim))
    return gain


def noise(stream_key, shape, scale, bound, pieces=(), kind=jnp.bfloat16):
    entries = scale * jax.random.normal(stream_key, shape, jnp.float32)
    if pieces:
        entries = entries * levels(stream_key, shape, pieces, -0.22, 0.18)
    return jnp.clip(entries, -bound, bound).astype(kind)


def setup_inputs(seed: int = 0) -> dict:
    seeds = jax.random.split(jax.random.key(seed), 5)
    spectral = noise(seeds[0], (WSLOTS, FOLD, 2 * LAYERS), 0.03, 0.1796875, ((0, 8), (2, 4)))
    legendre = noise(seeds[1], (WSLOTS, FOLD, NROWS), (WAVES // 2) ** -0.5, 0.4375, ((0, 8), (2, 4)))
    wave_pair = draw_wave_pair(jax.random.fold_in(seeds[4], 71), 0)
    lat_slot = draw_lat_slot(jax.random.fold_in(seeds[4], 71), 0)
    return {"spectral": spectral, "legendre": legendre, "wave_pair": wave_pair, "lat_slot": lat_slot}


def fold_masks(pair_ids, fold_count, wave_count):
    fold_rows = jnp.arange(fold_count, dtype=jnp.int32)
    filled = pair_ids >= 0
    border = wave_count - pair_ids
    lower = filled[:, None] & (fold_rows[None, :] < border[:, None])
    upper = filled[:, None] & (fold_rows[None, :] >= border[:, None])
    return jnp.stack([lower, upper], axis=1)


def trig_parts(wave_numbers, steps, counts_b):
    residue = (wave_numbers[None, None] * steps[None, :, None, None]) % counts_b
    angles = residue.astype(jnp.float32) * (2.0 * math.pi) / counts_b.astype(jnp.float32)
    return jnp.cos(angles), jnp.sin(angles)


def synthesis_table(pair_ids, row_lats, lat_count, lon_width, wave_count):
    filled = pair_ids >= 0
    wave_numbers = jnp.stack([pair_ids, wave_count - 1 - pair_ids], axis=1)
    lon_count = 20 + 4 * jnp.minimum(row_lats, lat_count - 1 - row_lats)
    highest = jnp.minimum(wave_count - 1, (lon_count - 1) // 2)
    counts_b = lon_count[:, None, None, None]
    coarse_count = (lon_width + 63) // 64
    coarse_steps = jnp.arange(coarse_count, dtype=jnp.int32) * 64
    fine_steps = jnp.arange(64, dtype=jnp.int32)
    cos_coarse, sin_coarse = trig_parts(wave_numbers, coarse_steps, counts_b)
    cos_fine, sin_fine = trig_parts(wave_numbers, fine_steps, counts_b)
    cos_all = cos_coarse[:, :, None] * cos_fine[:, None] - sin_coarse[:, :, None] * sin_fine[:, None]
    sin_all = sin_coarse[:, :, None] * cos_fine[:, None] + cos_coarse[:, :, None] * sin_fine[:, None]
    row_total = row_lats.shape[0]
    cos_all = cos_all.reshape(row_total, coarse_count * 64, wave_numbers.shape[0], 2)[:, :lon_width]
    sin_all = sin_all.reshape(row_total, coarse_count * 64, wave_numbers.shape[0], 2)[:, :lon_width]
    columns = jnp.arange(lon_width, dtype=jnp.int32)
    valid = filled[None, None, :, None] & (wave_numbers[None, None] <= highest[:, None, None, None]) & (columns[None, :, None, None] < counts_b)
    factor = jnp.where(wave_numbers == 0, 1.0, 2.0).astype(jnp.float32)[None, None]
    real_part = jnp.where(valid, factor * cos_all, 0.0)
    imag_part = jnp.where(valid, -factor * sin_all, 0.0)
    return jnp.stack([real_part, imag_part], axis=-1).astype(jnp.bfloat16)


def reference(spectral, legendre, wave_pair, lat_slot):
    fold_count = spectral.shape[1]
    wave_count = fold_count - 1
    lat_count = NLAT
    lon_width = 2 * lat_count + 16
    layer_count = spectral.shape[2] // 2
    row_total = lat_slot.shape[0]
    half_masks = fold_masks(wave_pair, fold_count, wave_count)
    paired = spectral.reshape(spectral.shape[0], fold_count, layer_count, 2)

    def per_slot(args):
        coefficients, weights, masks_one = args
        masked = jnp.where(masks_one[:, :, None, None], coefficients.astype(jnp.float32)[None], 0.0)
        summed = jnp.einsum("htlc,ta->ahcl", masked, weights.astype(jnp.float32))
        return summed.astype(jnp.bfloat16)

    fourier = lax.map(per_slot, (paired, legendre, half_masks))

    def per_row(args):
        latitude, position = args
        basis = synthesis_table(wave_pair, latitude[None], lat_count, lon_width, wave_count)[0]
        picked = jnp.take(fourier, position, axis=1)
        flat_basis = basis.reshape(lon_width, -1).astype(jnp.float32)
        flat_values = picked.reshape(-1, layer_count).astype(jnp.float32)
        result = jnp.dot(flat_basis, flat_values, preferred_element_type=jnp.float32)
        return result.T.astype(jnp.bfloat16)

    positions = jnp.arange(row_total, dtype=jnp.int32)
    return lax.map(per_row, (lat_slot, positions))
```

```python
import functools
import math

import jax
import jax.numpy as jnp
from jax import lax
from jax.experimental import pallas as pl
from jax.experimental.pallas import tpu as pltpu
from jax.sharding import PartitionSpec as P

NLAT = 800
LANE = 128
PACK = 4
HALVES = 2
SIDE = HALVES * PACK
KB = 64
ROW_STEP = 4
COLS = 256


def half_turn(x):
    u = x * math.pi
    v = u * u
    s = -2.5052108385441720e-08
    for coef in (2.7557319223985893e-06, -1.9841269841269841e-04, 8.3333333333333333e-03, -1.6666666666666667e-01, 1.0):
        s = s * v + coef
    s = s * u
    c = -2.7557319223985888e-07
    for coef in (2.4801587301587302e-05, -1.3888888888888889e-03, 4.1666666666666667e-02, -0.5, 1.0):
        c = c * v + coef
    return 1.0 - 2.0 * s * s, 2.0 * s * c


def trig(prod, count, inv):
    r = prod - jnp.floor(prod * inv + 0.5) * count
    return half_turn(r * inv)


def chunk_plan(slots, per_tile):
    bounds = []
    for lo in range(0, slots, per_tile):
        hi = min(slots, lo + per_tile)
        for start in range(lo, hi, PACK):
            bounds.append((start, min(hi, start + PACK)))
    return bounds


def group_plan(chunks):
    paired = max(0, chunks - 3) // 2 * 2
    return [(c, c + 1) for c in range(0, paired, 2)] + [(c,) for c in range(paired, chunks)]


def exchange_order(nw):
    if nw & (nw - 1):
        return list(range(1, nw))
    return sorted(range(1, nw), key=lambda k: (-bin(k >> 1).count("1"), k))


def partner(wi, k, nw, sending):
    if nw & (nw - 1):
        return lax.rem(wi + (k if sending else nw - k), nw)
    other = wi
    bit = 1
    while bit < nw:
        if k & bit:
            other = other + bit * (1 - 2 * lax.rem(lax.div(wi, bit), 2))
        bit *= 2
    return other


def kernel(
    nw, nl, slots, wave_count, bounds, groups, per_tile,
    wp_hbm, lat_hbm, spec_hbm, leg_hbm, out_ref,
    wp, lat, spec, own, leg, tail, wts, waves, stage, snd, rcv, basis, part,
    loc_sem, ag_send, ag_recv, aa_send, aa_recv,
):
    wi = lax.axis_index("wav")
    li = lax.axis_index("lev")
    chunks = len(bounds)
    rows, layers, width = out_ref.shape
    fold = spec.shape[1]
    main = leg.shape[3]
    rest = fold - main
    items = 2 * layers
    full = basis.shape[2]
    blocks = full // LANE
    kchunk = nw * SIDE
    qtot = nw * rows
    fmt = pl.DeviceIdType.MESH
    half = jnp.bfloat16

    copies = [
        pltpu.make_async_copy(src, dst, loc_sem.at[i])
        for i, (src, dst) in enumerate((
            (leg_hbm.at[:, :, pl.ds(0, main)], leg.at[li]),
            (leg_hbm, own),
            (wp_hbm, wp),
            (lat_hbm, lat),
            (spec_hbm, spec),
        ))
    ]
    for copy in copies:
        copy.start()
    leg_copy, own_copy, wp_copy, lat_copy, spec_copy = copies

    barrier = pltpu.get_barrier_semaphore()
    for step in (1, -1):
        @pl.when((li + step >= 0) & (li + step < nl))
        def _():
            pl.semaphore_signal(barrier, inc=1, device_id=(wi, li + step), device_id_type=fmt)
    order = exchange_order(nw)
    for k in order:
        pl.semaphore_signal(barrier, inc=1, device_id=(partner(wi, k, nw, True), li), device_id_type=fmt)
    beside = jnp.where(li > 0, 1, 0) + jnp.where(li < nl - 1, 1, 0)
    pl.semaphore_wait(barrier, beside + nw - 1)

    def fresh(c):
        lo, hi = bounds[c]
        return [t for t in range(tail.shape[1]) if lo <= t * per_tile < hi]

    def hops(way, k, c, block):
        lo, hi = bounds[c]
        views = [leg.at[block, pl.ds(lo, hi - lo)]] + [tail.at[block, t] for t in fresh(c)]
        return [
            pltpu.make_async_remote_copy(
                src_ref=view,
                dst_ref=view,
                send_sem=ag_send.at[way, k, c, n],
                recv_sem=ag_recv.at[way, k, c, n],
                device_id=(wi, li + 1 - 2 * way),
                device_id_type=fmt,
            )
            for n, view in enumerate(views)
        ]

    def sends(way, k):
        if way == 0:
            return (li - k >= 0) & (li + 1 < nl), jnp.maximum(li - k, 0)
        return (li + k < nl) & (li >= 1), jnp.minimum(li + k, nl - 1)

    def receives(way, k):
        if way == 0:
            return li - 1 - k >= 0, jnp.maximum(li - 1 - k, 0)
        return li + 1 + k < nl, jnp.minimum(li + 1 + k, nl - 1)

    def send(k, c, which=slice(None)):
        for way in range(2):
            going, block = sends(way, k)

            @pl.when(going)
            def _():
                for hop in hops(way, k, c, block)[which]:
                    hop.start()

    def arrive(k, c):
        for way in range(2):
            coming, block = receives(way, k)

            @pl.when(coming)
            def _():
                for hop in hops(way, k, c, block):
                    hop.wait_recv()

        if k + 1 < nl - 1:
            send(k + 1, c)

    def exchange(c, k):
        dest = partner(wi, k, nw, True)
        return pltpu.make_async_remote_copy(
            src_ref=snd.at[c, dest],
            dst_ref=rcv.at[c, wi],
            send_sem=aa_send.at[c, k],
            recv_sem=aa_recv.at[c, k],
            device_id=(dest, li),
            device_id_type=fmt,
        )

    leg_copy.wait()
    send(0, 0, slice(0, 1))
    own_copy.wait()
    place_t = lax.broadcasted_iota(jnp.int32, (rest, LANE), 0)
    place_x = lax.broadcasted_iota(jnp.int32, (rest, LANE), 1)
    for t in range(tail.shape[1]):
        total = jnp.zeros(tail.shape[2:], jnp.float32)
        for n in range(per_tile):
            s = t * per_tile + n
            if s < slots:
                place = jnp.where(place_x == place_t + n * rest, 1.0, 0.0).astype(half)
                total += jnp.dot(own[s, :, main:], place, preferred_element_type=jnp.float32)
        tail[li, t] = total.astype(half)
    send(0, 0, slice(1, None))
    ahead = chunks // 2 + 1
    for c in range(1, ahead):
        send(0, c)

    waves[...] = jnp.full_like(waves, -1.0)
    wp_copy.wait()
    lat_copy.wait()

    def place_waves(src, carry):
        for c, (lo, hi) in enumerate(bounds):
            for s in range(lo, hi):
                p = wp[src * slots + s]
                for h in range(HALVES):
                    m = jnp.where(p < 0, -1, p if h == 0 else wave_count - 1 - p).astype(jnp.float32)
                    row = c * kchunk + src * SIDE + h * PACK + s - lo
                    waves[pl.ds(row, 1), :] = jnp.full((1, LANE), m, jnp.float32)
        return carry

    lax.fori_loop(0, nw, place_waves, 0)

    stage[...] = jnp.zeros_like(stage)
    out_i = lax.broadcasted_iota(jnp.int32, (items, items), 1)
    in_i = lax.broadcasted_iota(jnp.int32, (items, items), 0)
    perm = jnp.where(
        in_i == jnp.where(out_i < layers, 2 * out_i, 2 * (out_i - layers) + 1), 1.0, 0.0
    ).astype(half)
    back_x = lax.broadcasted_iota(jnp.int32, (LANE, rest), 0)
    back_t = lax.broadcasted_iota(jnp.int32, (LANE, rest), 1)

    def weigh(s, carry):
        n = lax.rem(s, per_tile)
        wts[s, :main, :] = jnp.dot(spec[s, :main, :], perm, preferred_element_type=jnp.float32).astype(half)
        back = jnp.where(back_x == back_t + n * rest, 1.0, 0.0).astype(half)
        tails = jnp.dot(spec[s, main:, :], perm, preferred_element_type=jnp.float32).astype(half)
        wts[s, main:, :] = jnp.dot(back, tails, preferred_element_type=jnp.float32).astype(half)
        return carry

    fine = lax.broadcasted_iota(jnp.int32, (KB, LANE), 1).astype(jnp.float32)
    lane = lax.broadcasted_iota(jnp.int32, (KB, LANE), 1)
    pieces = kchunk // KB
    steps = rows // ROW_STEP

    def row_count(r):
        a = lat[wi * rows + r]
        return 20 + 4 * jnp.minimum(a, NLAT - 1 - a)

    def basis_rows(c):
        for group, start in zip(groups, group_starts):
            if c in group:
                real = start + group.index(c) * kchunk
                return real, real + len(group) * kchunk

    group_starts = []
    for group in groups:
        group_starts.append(2 * kchunk * sum(len(g) for g in groups[: len(group_starts)]))

    def make_basis(c, unit):
        real0, imag0 = basis_rows(c)
        piece = lax.div(unit, steps)
        r0 = lax.rem(unit, steps) * ROW_STEP
        k0 = pl.multiple_of(piece * KB, KB)
        m = waves[pl.ds(pl.multiple_of(c * kchunk + k0, KB), KB), :]
        counts = [row_count(r0 + i) for i in range(ROW_STEP)]
        each = jnp.full((KB, LANE), counts[0].astype(jnp.float32), jnp.float32)
        for i in range(1, ROW_STEP):
            each = jnp.where(lane == i, counts[i].astype(jnp.float32), each)
        stride_cos, stride_sin = trig(m * LANE, each, 1.0 / each)
        for i in range(ROW_STEP):
            r = r0 + i
            highest = jnp.minimum(wave_count - 1, lax.shift_right_logical(counts[i] - 1, 1)).astype(jnp.float32)
            count = jnp.full((KB, LANE), counts[i].astype(jnp.float32), jnp.float32)
            factor = jnp.where((m >= 0.0) & (m <= highest), jnp.where(m == 0.0, 1.0, 2.0), 0.0)
            sc = jnp.broadcast_to(stride_cos[:, i : i + 1], (KB, LANE))
            ss = jnp.broadcast_to(stride_sin[:, i : i + 1], (KB, LANE))
            c0, s0 = trig(m * fine, count, 1.0 / count)
            c0 = c0 * factor
            s0 = -(s0 * factor)
            c1 = c0 * sc + s0 * ss
            s1 = s0 * sc - c0 * ss
            twice = sc + sc
            for b in range(blocks):
                cols = slice(b * LANE, (b + 1) * LANE)
                basis[r, pl.ds(real0 + k0, KB), cols] = c0.astype(half)
                basis[r, pl.ds(imag0 + k0, KB), cols] = s0.astype(half)
                if b + 1 < blocks:
                    c0, c1 = c1, twice * c1 - c0
                    s0, s1 = s1, twice * s1 - s0

    def basis_for(c):
        def body(unit, carry):
            make_basis(c, unit)
            return carry

        lax.fori_loop(0, pieces * steps, body, 0)

    cols = lax.broadcasted_iota(jnp.int32, (1, main), 1)
    tcols = lax.broadcasted_iota(jnp.int32, (1, LANE), 1)

    def fourier(c):
        lo, hi = bounds[c]
        for s in range(lo, hi):
            border = wave_count - wp[wi * slots + s]
            fold_rows = jnp.concatenate([cols, main + tcols - s % per_tile * rest], axis=1)
            low = jnp.where(fold_rows < border, 1.0, 0.0).astype(half)
            values = jnp.concatenate([
                leg[:, s].reshape(qtot, main),
                tail[:, s // per_tile].reshape(qtot, LANE),
            ], axis=1)
            picked = values * low
            f = jnp.dot(
                jnp.concatenate([picked, values - picked], axis=0), wts[s],
                preferred_element_type=jnp.float32,
            )
            for h in range(HALVES):
                stage[pl.ds(h * PACK + s - lo, qtot, stride=SIDE), :] = f[h * qtot : (h + 1) * qtot]
        snd[c] = stage[...].astype(half).reshape(snd.shape[1:])
        for k in order:
            exchange(c, k).start()
        mine = stage[pl.ds(pl.multiple_of(wi * rows * SIDE, rows * SIDE), rows * SIDE), :]
        rcv[c, wi] = mine.astype(half).reshape(rcv.shape[2:])

    def landed(c):
        for k in order:
            exchange(c, k).wait_recv()

    lanes = lax.broadcasted_iota(jnp.int32, (layers, COLS), 1)

    def synthesis(g):
        group = groups[g]
        for c in group:
            landed(c)
        depth = 2 * kchunk * len(group)

        def body(r, carry):
            v = jnp.concatenate([rcv[c, :, r].reshape(kchunk, items) for c in group], axis=0)
            vt = v.T
            lhs = jnp.concatenate([vt[:layers], vt[layers:]], axis=1)
            count = row_count(r)
            for n0 in range(0, full, COLS):
                n1 = min(full, n0 + COLS)
                rhs = basis[r, group_starts[g] : group_starts[g] + depth, n0:n1]
                value = jnp.dot(lhs, rhs, preferred_element_type=jnp.float32)
                if g:
                    value = part[r, :, n0:n1] + value
                if g + 1 < len(groups):
                    part[r, :, n0:n1] = value
                else:
                    value = jnp.where(lanes[:, : n1 - n0] + n0 < count, value, 0.0)
                    stop = min(width, n1)
                    out_ref[r, :, n0:stop] = value[:, : stop - n0].astype(half)
            return carry

        lax.fori_loop(0, rows, body, 0, unroll=2)

    spec_copy.wait()
    lax.fori_loop(0, slots, weigh, 0)

    polls = sorted(((k, c) for k in range(nl - 1) for c in range(chunks)), key=lambda p: (p[0] + p[1], p[0]))
    made = 0
    ready = 0
    shown = 0
    for k, c in polls:
        arrive(k, c)
        if k == 0 and ahead < chunks:
            send(0, ahead)
            ahead += 1
        if k == nl - 2:
            fourier(c)
            ready = c + 1
            while shown < len(groups) and groups[shown][-1] + 3 <= c:
                synthesis(shown)
                shown += 1
        if made < chunks:
            basis_for(made)
            made += 1
    while made < chunks:
        basis_for(made)
        made += 1
    while shown < len(groups):
        synthesis(shown)
        shown += 1

    for c in range(chunks):
        for k in range(nl - 1):
            for way in range(2):
                going, block = sends(way, k)

                @pl.when(going)
                def _():
                    for hop in hops(way, k, c, block):
                        hop.wait_send()

        for k in order:
            exchange(c, k).wait_send()


def on_device(spectral, legendre, wave_pair, lat_slot):
    slots, fold, items = spectral.shape
    wave_count = fold - 1
    nw = lax.axis_size("wav")
    nl = lax.axis_size("lev")
    rows = lat_slot.shape[0] // nw
    layers = items // 2
    width = 2 * NLAT + 16
    full = -(-width // LANE) * LANE
    main = fold // LANE * LANE
    per_tile = LANE // (fold - main)
    bounds = chunk_plan(slots, per_tile)
    chunks = len(bounds)
    groups = group_plan(chunks)
    tiles = -(-slots // per_tile)
    leg_t = jnp.transpose(legendre, (0, 2, 1))
    lrows = leg_t.shape[1]
    kchunk = nw * SIDE

    hbm = pl.BlockSpec(memory_space=pl.ANY)
    dma = pltpu.SemaphoreType.DMA
    vmem = pltpu.VMEM
    half = jnp.bfloat16
    place = functools.partial(pltpu.with_memory_space_constraint, memory_space=pltpu.HBM)
    return pl.pallas_call(
        functools.partial(kernel, nw, nl, slots, wave_count, bounds, groups, per_tile),
        out_shape=vmem((rows, layers, width), half),
        in_specs=[hbm, hbm, hbm, hbm],
        out_specs=pl.BlockSpec(memory_space=vmem),
        scratch_shapes=[
            pltpu.SMEM(wave_pair.shape, jnp.int32),
            pltpu.SMEM(lat_slot.shape, jnp.int32),
            vmem((slots, fold, items), half),
            vmem((slots, lrows, fold), half),
            vmem((nl, slots, lrows, main), half),
            vmem((nl, tiles, lrows, LANE), half),
            vmem((slots, main + LANE, items), half),
            vmem((chunks * kchunk, LANE), jnp.float32),
            vmem((nw * rows * SIDE, items), jnp.float32),
            vmem((chunks, nw, rows, SIDE, items), half),
            vmem((chunks, nw, rows, SIDE, items), half),
            vmem((rows, 2 * chunks * kchunk, full), half),
            vmem((rows, layers, full), jnp.float32),
            dma((5,)),
            dma((2, nl - 1, chunks, 2)),
            dma((2, nl - 1, chunks, 2)),
            dma((chunks, nw)),
            dma((chunks, nw)),
        ],
        compiler_params=pltpu.CompilerParams(collective_id=0, has_side_effects=True, vmem_limit_bytes=52 << 20),
    )(place(wave_pair), place(lat_slot), place(spectral), place(leg_t))


def solution(mesh):
    return jax.shard_map(
        on_device,
        mesh=mesh,
        in_specs=(P("wav", None, "lev"), P("wav", None, "lev"), P(), P()),
        out_specs=P("wav", "lev", None),
        check_vma=False,
    )
```

```python
import functools
import math

import jax
import jax.numpy as jnp
from jax import lax
from jax.experimental import pallas as pl
from jax.experimental.pallas import tpu as pltpu
from jax.sharding import PartitionSpec as P

NLAT = 800
LANE = 128
PACK = 4
HALVES = 2
SIDE = HALVES * PACK
KB = 64
ROW_STEP = 4
COLS = 256


def half_turn(x):
    u = x * math.pi
    v = u * u
    s = -2.5052108385441720e-08
    for coef in (2.7557319223985893e-06, -1.9841269841269841e-04, 8.3333333333333333e-03, -1.6666666666666667e-01, 1.0):
        s = s * v + coef
    s = s * u
    c = -2.7557319223985888e-07
    for coef in (2.4801587301587302e-05, -1.3888888888888889e-03, 4.1666666666666667e-02, -0.5, 1.0):
        c = c * v + coef
    return 1.0 - 2.0 * s * s, 2.0 * s * c


def trig(prod, count, inv):
    r = prod - jnp.floor(prod * inv + 0.5) * count
    return half_turn(r * inv)


def chunk_plan(slots, per_tile):
    bounds = []
    for lo in range(0, slots, per_tile):
        hi = min(slots, lo + per_tile)
        for start in range(lo, hi, PACK):
            bounds.append((start, min(hi, start + PACK)))
    return bounds


def group_plan(chunks):
    paired = max(0, chunks - 3) // 2 * 2
    return [(c, c + 1) for c in range(0, paired, 2)] + [(c,) for c in range(paired, chunks)]


def exchange_order(nw):
    if nw & (nw - 1):
        return list(range(1, nw))
    return sorted(range(1, nw), key=lambda k: (-bin(k >> 1).count("1"), k))


def partner(wi, k, nw, sending):
    if nw & (nw - 1):
        return lax.rem(wi + (k if sending else nw - k), nw)
    other = wi
    bit = 1
    while bit < nw:
        if k & bit:
            other = other + bit * (1 - 2 * lax.rem(lax.div(wi, bit), 2))
        bit *= 2
    return other


def kernel(
    nw, nl, slots, wave_count, bounds, groups, per_tile,
    wp_hbm, lat_hbm, spec_hbm, leg_hbm, out_ref,
    wp, lat, spec, own, leg, tail, wts, waves, stage, snd, rcv, basis, part,
    loc_sem, ag_send, ag_recv, aa_send, aa_recv,
):
    wi = lax.axis_index("wav")
    li = lax.axis_index("lev")
    chunks = len(bounds)
    rows, layers, width = out_ref.shape
    fold = spec.shape[1]
    main = leg.shape[3]
    rest = fold - main
    items = 2 * layers
    full = basis.shape[2]
    blocks = full // LANE
    kchunk = nw * SIDE
    qtot = nw * rows
    fmt = pl.DeviceIdType.MESH
    half = jnp.bfloat16

    copies = [
        pltpu.make_async_copy(src, dst, loc_sem.at[i])
        for i, (src, dst) in enumerate((
            (leg_hbm.at[:, :, pl.ds(0, main)], leg.at[li]),
            (leg_hbm, own),
            (wp_hbm, wp),
            (lat_hbm, lat),
            (spec_hbm, spec),
        ))
    ]
    for copy in copies:
        copy.start()
    leg_copy, own_copy, wp_copy, lat_copy, spec_copy = copies

    barrier = pltpu.get_barrier_semaphore()
    for step in (1, -1):
        @pl.when((li + step >= 0) & (li + step < nl))
        def _():
            pl.semaphore_signal(barrier, inc=1, device_id=(wi, li + step), device_id_type=fmt)
    order = exchange_order(nw)
    for k in order:
        pl.semaphore_signal(barrier, inc=1, device_id=(partner(wi, k, nw, True), li), device_id_type=fmt)
    beside = jnp.where(li > 0, 1, 0) + jnp.where(li < nl - 1, 1, 0)
    pl.semaphore_wait(barrier, beside + nw - 1)

    def fresh(c):
        lo, hi = bounds[c]
        return [t for t in range(tail.shape[1]) if lo <= t * per_tile < hi]

    def hops(way, k, c, block, pieces=(0, 1)):
        lo, hi = bounds[c]
        views = [(0, leg.at[block, pl.ds(lo, hi - lo)])] + [(1, tail.at[block, t]) for t in fresh(c)]
        return [
            pltpu.make_async_remote_copy(
                src_ref=view,
                dst_ref=view,
                send_sem=ag_send.at[way, k, c, n],
                recv_sem=ag_recv.at[way, k, c, n],
                device_id=(wi, li + 1 - 2 * way),
                device_id_type=fmt,
            )
            for n, view in views
            if n in pieces
        ]

    def sends(way, k):
        if way == 0:
            return (li - k >= 0) & (li + 1 < nl), jnp.maximum(li - k, 0)
        return (li + k < nl) & (li >= 1), jnp.minimum(li + k, nl - 1)

    def receives(way, k):
        if way == 0:
            return li - 1 - k >= 0, jnp.maximum(li - 1 - k, 0)
        return li + 1 + k < nl, jnp.minimum(li + 1 + k, nl - 1)

    def send(k, c, pieces=(0, 1)):
        for way in range(2):
            going, block = sends(way, k)

            @pl.when(going)
            def _():
                for hop in hops(way, k, c, block, pieces):
                    hop.start()

    def arrive(k, c):
        for way in range(2):
            coming, block = receives(way, k)

            @pl.when(coming)
            def _():
                for hop in hops(way, k, c, block):
                    hop.wait_recv()

        if k + 1 < nl - 1:
            send(k + 1, c)

    def exchange(c, k):
        dest = partner(wi, k, nw, True)
        return pltpu.make_async_remote_copy(
            src_ref=snd.at[c, dest],
            dst_ref=rcv.at[c, wi],
            send_sem=aa_send.at[c, k],
            recv_sem=aa_recv.at[c, k],
            device_id=(dest, li),
            device_id_type=fmt,
        )

    leg_copy.wait()
    send(0, 0, (0,))
    own_copy.wait()
    place_t = lax.broadcasted_iota(jnp.int32, (rest, LANE), 0)
    place_x = lax.broadcasted_iota(jnp.int32, (rest, LANE), 1)
    for t in range(tail.shape[1]):
        total = jnp.zeros(tail.shape[2:], jnp.float32)
        for n in range(per_tile):
            s = t * per_tile + n
            if s < slots:
                place = jnp.where(place_x == place_t + n * rest, 1.0, 0.0).astype(half)
                total += jnp.dot(own[s, :, main:], place, preferred_element_type=jnp.float32)
        tail[li, t] = total.astype(half)
    send(0, 0, (1,))
    ahead = min(chunks, 3)
    for c in range(1, ahead):
        send(0, c)

    waves[...] = jnp.full_like(waves, -1.0)
    wp_copy.wait()
    lat_copy.wait()

    def place_waves(src, carry):
        for c, (lo, hi) in enumerate(bounds):
            for s in range(lo, hi):
                p = wp[src * slots + s]
                for h in range(HALVES):
                    m = jnp.where(p < 0, -1, p if h == 0 else wave_count - 1 - p).astype(jnp.float32)
                    row = c * kchunk + src * SIDE + h * PACK + s - lo
                    waves[pl.ds(row, 1), :] = jnp.full((1, LANE), m, jnp.float32)
        return carry

    lax.fori_loop(0, nw, place_waves, 0)

    stage[...] = jnp.zeros_like(stage)
    out_i = lax.broadcasted_iota(jnp.int32, (items, items), 1)
    in_i = lax.broadcasted_iota(jnp.int32, (items, items), 0)
    perm = jnp.where(
        in_i == jnp.where(out_i < layers, 2 * out_i, 2 * (out_i - layers) + 1), 1.0, 0.0
    ).astype(half)
    back_x = lax.broadcasted_iota(jnp.int32, (LANE, rest), 0)
    back_t = lax.broadcasted_iota(jnp.int32, (LANE, rest), 1)

    def weigh(s):
        n = s % per_tile
        wts[s, :main, :] = jnp.dot(spec[s, :main, :], perm, preferred_element_type=jnp.float32).astype(half)
        back = jnp.where(back_x == back_t + n * rest, 1.0, 0.0).astype(half)
        tails = jnp.dot(spec[s, main:, :], perm, preferred_element_type=jnp.float32).astype(half)
        wts[s, main:, :] = jnp.dot(back, tails, preferred_element_type=jnp.float32).astype(half)

    fine = lax.broadcasted_iota(jnp.int32, (KB, LANE), 1).astype(jnp.float32)
    lane = lax.broadcasted_iota(jnp.int32, (KB, LANE), 1)
    pieces = kchunk // KB
    steps = rows // ROW_STEP

    def row_count(r):
        a = lat[wi * rows + r]
        return 20 + 4 * jnp.minimum(a, NLAT - 1 - a)

    def basis_rows(c):
        for group, start in zip(groups, group_starts):
            if c in group:
                real = start + group.index(c) * kchunk
                return real, real + len(group) * kchunk

    group_starts = []
    for group in groups:
        group_starts.append(2 * kchunk * sum(len(g) for g in groups[: len(group_starts)]))

    def make_basis(c, unit):
        real0, imag0 = basis_rows(c)
        k0 = unit // steps * KB
        r0 = unit % steps * ROW_STEP
        m = waves[c * kchunk + k0 : c * kchunk + k0 + KB, :]
        counts = [row_count(r0 + i) for i in range(ROW_STEP)]
        each = jnp.full((KB, LANE), counts[0].astype(jnp.float32), jnp.float32)
        for i in range(1, ROW_STEP):
            each = jnp.where(lane == i, counts[i].astype(jnp.float32), each)
        stride_cos, stride_sin = trig(m * LANE, each, 1.0 / each)
        for i in range(ROW_STEP):
            r = r0 + i
            highest = jnp.minimum(wave_count - 1, lax.shift_right_logical(counts[i] - 1, 1)).astype(jnp.float32)
            count = jnp.full((KB, LANE), counts[i].astype(jnp.float32), jnp.float32)
            factor = jnp.where((m >= 0.0) & (m <= highest), jnp.where(m == 0.0, 1.0, 2.0), 0.0)
            sc = jnp.broadcast_to(stride_cos[:, i : i + 1], (KB, LANE))
            ss = jnp.broadcast_to(stride_sin[:, i : i + 1], (KB, LANE))
            c0, s0 = trig(m * fine, count, 1.0 / count)
            c0 = c0 * factor
            s0 = -(s0 * factor)
            c1 = c0 * sc + s0 * ss
            s1 = s0 * sc - c0 * ss
            twice = sc + sc
            for b in range(blocks):
                cols = slice(b * LANE, (b + 1) * LANE)
                basis[r, real0 + k0 : real0 + k0 + KB, cols] = c0.astype(half)
                basis[r, imag0 + k0 : imag0 + k0 + KB, cols] = s0.astype(half)
                if b + 1 < blocks:
                    c0, c1 = c1, twice * c1 - c0
                    s0, s1 = s1, twice * s1 - s0

    cols = lax.broadcasted_iota(jnp.int32, (1, main), 1)
    tcols = lax.broadcasted_iota(jnp.int32, (1, LANE), 1)

    def fourier(c):
        lo, hi = bounds[c]
        for s in range(lo, hi):
            border = wave_count - wp[wi * slots + s]
            fold_rows = jnp.concatenate([cols, main + tcols - s % per_tile * rest], axis=1)
            low = jnp.where(fold_rows < border, 1.0, 0.0).astype(half)
            values = jnp.concatenate([
                leg[:, s].reshape(qtot, main),
                tail[:, s // per_tile].reshape(qtot, LANE),
            ], axis=1)
            picked = values * low
            f = jnp.dot(
                jnp.concatenate([picked, values - picked], axis=0), wts[s],
                preferred_element_type=jnp.float32,
            )
            for h in range(HALVES):
                stage[pl.ds(h * PACK + s - lo, qtot, stride=SIDE), :] = f[h * qtot : (h + 1) * qtot]
        snd[c] = stage[...].astype(half).reshape(snd.shape[1:])
        for k in order:
            exchange(c, k).start()
        mine = stage[pl.ds(pl.multiple_of(wi * rows * SIDE, rows * SIDE), rows * SIDE), :]
        rcv[c, wi] = mine.astype(half).reshape(rcv.shape[2:])

    def landed(c):
        for k in order:
            exchange(c, k).wait_recv()

    lanes = lax.broadcasted_iota(jnp.int32, (layers, COLS), 1)

    def synthesis(g):
        group = groups[g]
        for c in group:
            landed(c)
        depth = 2 * kchunk * len(group)

        def body(r, carry):
            v = jnp.concatenate([rcv[c, :, r].reshape(kchunk, items) for c in group], axis=0)
            vt = v.T
            lhs = jnp.concatenate([vt[:layers], vt[layers:]], axis=1)
            count = row_count(r)
            for n0 in range(0, full, COLS):
                n1 = min(full, n0 + COLS)
                rhs = basis[r, group_starts[g] : group_starts[g] + depth, n0:n1]
                value = jnp.dot(lhs, rhs, preferred_element_type=jnp.float32)
                if g:
                    value = part[r, :, n0:n1] + value
                if g + 1 < len(groups):
                    part[r, :, n0:n1] = value
                else:
                    value = jnp.where(lanes[:, : n1 - n0] + n0 < count, value, 0.0)
                    stop = min(width, n1)
                    out_ref[r, :, n0:stop] = value[:, : stop - n0].astype(half)
            return carry

        lax.fori_loop(0, rows, body, 0, unroll=2)

    units = [(c, unit) for c in range(chunks) for unit in range(pieces * steps)]
    pace = -(-slots // len(units))
    done = {"weighed": 0, "made": 0}

    def prepare(upto):
        while done["weighed"] < min(slots, upto):
            weigh(done["weighed"])
            done["weighed"] += 1

    def work(upto):
        while done["made"] < min(len(units), upto):
            prepare(done["weighed"] + pace)
            make_basis(*units[done["made"]])
            done["made"] += 1

    spec_copy.wait()
    polls = sorted(((k, c) for k in range(nl - 1) for c in range(chunks)), key=lambda p: (p[0] + p[1], p[0]))
    shown = 0
    for k, c in polls:
        arrive(k, c)
        if k == 0 and ahead < chunks:
            send(0, ahead)
            ahead += 1
        if k == nl - 2:
            prepare(bounds[c][1])
            fourier(c)
            while shown < len(groups) and groups[shown][-1] + 3 <= c:
                work(len(units) // chunks * (groups[shown][-1] + 1))
                synthesis(shown)
                shown += 1
        work(done["made"] + 1)
    work(len(units))
    while shown < len(groups):
        synthesis(shown)
        shown += 1

    for c in range(chunks):
        for k in range(nl - 1):
            for way in range(2):
                going, block = sends(way, k)

                @pl.when(going)
                def _():
                    for hop in hops(way, k, c, block):
                        hop.wait_send()

        for k in order:
            exchange(c, k).wait_send()


def on_device(spectral, legendre, wave_pair, lat_slot):
    slots, fold, items = spectral.shape
    wave_count = fold - 1
    nw = lax.axis_size("wav")
    nl = lax.axis_size("lev")
    rows = lat_slot.shape[0] // nw
    layers = items // 2
    width = 2 * NLAT + 16
    full = -(-width // LANE) * LANE
    main = fold // LANE * LANE
    per_tile = LANE // (fold - main)
    bounds = chunk_plan(slots, per_tile)
    chunks = len(bounds)
    groups = group_plan(chunks)
    tiles = -(-slots // per_tile)
    leg_t = jnp.transpose(legendre, (0, 2, 1))
    lrows = leg_t.shape[1]
    kchunk = nw * SIDE

    hbm = pl.BlockSpec(memory_space=pl.ANY)
    dma = pltpu.SemaphoreType.DMA
    vmem = pltpu.VMEM
    half = jnp.bfloat16
    place = functools.partial(pltpu.with_memory_space_constraint, memory_space=pltpu.HBM)
    return pl.pallas_call(
        functools.partial(kernel, nw, nl, slots, wave_count, bounds, groups, per_tile),
        out_shape=vmem((rows, layers, width), half),
        in_specs=[hbm, hbm, hbm, hbm],
        out_specs=pl.BlockSpec(memory_space=vmem),
        scratch_shapes=[
            pltpu.SMEM(wave_pair.shape, jnp.int32),
            pltpu.SMEM(lat_slot.shape, jnp.int32),
            vmem((slots, fold, items), half),
            vmem((slots, lrows, fold), half),
            vmem((nl, slots, lrows, main), half),
            vmem((nl, tiles, lrows, LANE), half),
            vmem((slots, main + LANE, items), half),
            vmem((chunks * kchunk, LANE), jnp.float32),
            vmem((nw * rows * SIDE, items), jnp.float32),
            vmem((chunks, nw, rows, SIDE, items), half),
            vmem((chunks, nw, rows, SIDE, items), half),
            vmem((rows, 2 * chunks * kchunk, full), half),
            vmem((rows, layers, full), jnp.float32),
            dma((5,)),
            dma((2, nl - 1, chunks, 2)),
            dma((2, nl - 1, chunks, 2)),
            dma((chunks, nw)),
            dma((chunks, nw)),
        ],
        compiler_params=pltpu.CompilerParams(collective_id=0, has_side_effects=True, vmem_limit_bytes=52 << 20),
    )(place(wave_pair), place(lat_slot), place(spectral), place(leg_t))


def solution(mesh):
    return jax.shard_map(
        on_device,
        mesh=mesh,
        in_specs=(P("wav", None, "lev"), P("wav", None, "lev"), P(), P()),
        out_specs=P("wav", "lev", None),
        check_vma=False,
    )
```

```python
import functools
import math

import jax
import jax.numpy as jnp
from jax import lax
from jax.experimental import pallas as pl
from jax.experimental.pallas import tpu as pltpu
from jax.sharding import PartitionSpec as P

NLAT = 800
LANE = 128
PACK = 4
HALVES = 2
SIDE = HALVES * PACK
KB = 64
ROW_STEP = 4
COLS = 256


def half_turn(x):
    u = x * math.pi
    v = u * u
    s = -2.5052108385441720e-08
    for coef in (2.7557319223985893e-06, -1.9841269841269841e-04, 8.3333333333333333e-03, -1.6666666666666667e-01, 1.0):
        s = s * v + coef
    s = s * u
    c = -2.7557319223985888e-07
    for coef in (2.4801587301587302e-05, -1.3888888888888889e-03, 4.1666666666666667e-02, -0.5, 1.0):
        c = c * v + coef
    return 1.0 - 2.0 * s * s, 2.0 * s * c


def trig(prod, count, inv):
    r = prod - jnp.floor(prod * inv + 0.5) * count
    return half_turn(r * inv)


def chunk_plan(slots, per_tile):
    bounds = []
    for lo in range(0, slots, per_tile):
        hi = min(slots, lo + per_tile)
        for start in range(lo, hi, PACK):
            bounds.append((start, min(hi, start + PACK)))
    return bounds


def group_plan(chunks):
    paired = max(0, chunks - 3) // 2 * 2
    return [(c, c + 1) for c in range(0, paired, 2)] + [(c,) for c in range(paired, chunks)]


def exchange_order(nw):
    if nw & (nw - 1):
        return list(range(1, nw))
    return sorted(range(1, nw), key=lambda k: (-bin(k >> 1).count("1"), k))


def partner(wi, k, nw, sending):
    if nw & (nw - 1):
        return lax.rem(wi + (k if sending else nw - k), nw)
    other = wi
    bit = 1
    while bit < nw:
        if k & bit:
            other = other + bit * (1 - 2 * lax.rem(lax.div(wi, bit), 2))
        bit *= 2
    return other


def kernel(
    nw, nl, slots, wave_count, bounds, groups, per_tile,
    wp_hbm, lat_hbm, spec_hbm, leg_hbm, out_ref,
    wp, lat, spec, own, leg, tail, wts, waves, stage, snd, rcv, basis, part,
    loc_sem, ag_send, ag_recv, aa_send, aa_recv,
):
    wi = lax.axis_index("wav")
    li = lax.axis_index("lev")
    chunks = len(bounds)
    rows, layers, width = out_ref.shape
    fold = spec.shape[1]
    main = leg.shape[3]
    rest = fold - main
    items = 2 * layers
    blocks = basis.shape[1]
    full = blocks * LANE
    kchunk = nw * SIDE
    qtot = nw * rows
    fmt = pl.DeviceIdType.MESH
    half = jnp.bfloat16

    copies = [
        pltpu.make_async_copy(src, dst, loc_sem.at[i])
        for i, (src, dst) in enumerate((
            (leg_hbm.at[:, :, pl.ds(0, main)], leg.at[li]),
            (leg_hbm, own),
            (wp_hbm, wp),
            (lat_hbm, lat),
            (spec_hbm, spec),
        ))
    ]
    for copy in copies:
        copy.start()
    leg_copy, own_copy, wp_copy, lat_copy, spec_copy = copies

    barrier = pltpu.get_barrier_semaphore()
    for step in (1, -1):
        @pl.when((li + step >= 0) & (li + step < nl))
        def _():
            pl.semaphore_signal(barrier, inc=1, device_id=(wi, li + step), device_id_type=fmt)
    order = exchange_order(nw)
    for k in order:
        pl.semaphore_signal(barrier, inc=1, device_id=(partner(wi, k, nw, True), li), device_id_type=fmt)
    beside = jnp.where(li > 0, 1, 0) + jnp.where(li < nl - 1, 1, 0)
    pl.semaphore_wait(barrier, beside + nw - 1)

    def fresh(c):
        lo, hi = bounds[c]
        return [t for t in range(tail.shape[1]) if lo <= t * per_tile < hi]

    def hops(way, k, c, block, pieces=(0, 1)):
        lo, hi = bounds[c]
        views = [(0, leg.at[block, pl.ds(lo, hi - lo)])] + [(1, tail.at[block, t]) for t in fresh(c)]
        return [
            pltpu.make_async_remote_copy(
                src_ref=view,
                dst_ref=view,
                send_sem=ag_send.at[way, k, c, n],
                recv_sem=ag_recv.at[way, k, c, n],
                device_id=(wi, li + 1 - 2 * way),
                device_id_type=fmt,
            )
            for n, view in views
            if n in pieces
        ]

    def sends(way, k):
        if way == 0:
            return (li - k >= 0) & (li + 1 < nl), jnp.maximum(li - k, 0)
        return (li + k < nl) & (li >= 1), jnp.minimum(li + k, nl - 1)

    def receives(way, k):
        if way == 0:
            return li - 1 - k >= 0, jnp.maximum(li - 1 - k, 0)
        return li + 1 + k < nl, jnp.minimum(li + 1 + k, nl - 1)

    def send(k, c, pieces=(0, 1)):
        for way in range(2):
            going, block = sends(way, k)

            @pl.when(going)
            def _():
                for hop in hops(way, k, c, block, pieces):
                    hop.start()

    def arrive(k, c):
        for way in range(2):
            coming, block = receives(way, k)

            @pl.when(coming)
            def _():
                for hop in hops(way, k, c, block):
                    hop.wait_recv()

        if k + 1 < nl - 1:
            send(k + 1, c)

    def exchange(c, k):
        dest = partner(wi, k, nw, True)
        return pltpu.make_async_remote_copy(
            src_ref=snd.at[c, dest],
            dst_ref=rcv.at[c, wi],
            send_sem=aa_send.at[c, k],
            recv_sem=aa_recv.at[c, k],
            device_id=(dest, li),
            device_id_type=fmt,
        )

    leg_copy.wait()
    send(0, 0, (0,))
    own_copy.wait()
    place_t = lax.broadcasted_iota(jnp.int32, (rest, LANE), 0)
    place_x = lax.broadcasted_iota(jnp.int32, (rest, LANE), 1)
    for t in range(tail.shape[1]):
        total = jnp.zeros(tail.shape[2:], jnp.float32)
        for n in range(per_tile):
            s = t * per_tile + n
            if s < slots:
                place = jnp.where(place_x == place_t + n * rest, 1.0, 0.0).astype(half)
                total += jnp.dot(own[s, :, main:], place, preferred_element_type=jnp.float32)
        tail[li, t] = total.astype(half)
    send(0, 0, (1,))
    ahead = min(chunks, 3)
    for c in range(1, ahead):
        send(0, c)

    waves[...] = jnp.full_like(waves, -1.0)
    wp_copy.wait()
    lat_copy.wait()

    def place_waves(src, carry):
        for c, (lo, hi) in enumerate(bounds):
            for s in range(lo, hi):
                p = wp[src * slots + s]
                for h in range(HALVES):
                    m = jnp.where(p < 0, -1, p if h == 0 else wave_count - 1 - p).astype(jnp.float32)
                    row = c * kchunk + src * SIDE + h * PACK + s - lo
                    waves[pl.ds(row, 1), :] = jnp.full((1, LANE), m, jnp.float32)
        return carry

    lax.fori_loop(0, nw, place_waves, 0)

    stage[...] = jnp.zeros_like(stage)
    out_i = lax.broadcasted_iota(jnp.int32, (items, items), 1)
    in_i = lax.broadcasted_iota(jnp.int32, (items, items), 0)
    perm = jnp.where(
        in_i == jnp.where(out_i < layers, 2 * out_i, 2 * (out_i - layers) + 1), 1.0, 0.0
    ).astype(half)
    back_x = lax.broadcasted_iota(jnp.int32, (LANE, rest), 0)
    back_t = lax.broadcasted_iota(jnp.int32, (LANE, rest), 1)

    def weigh(s):
        n = s % per_tile
        wts[s, :main, :] = jnp.dot(spec[s, :main, :], perm, preferred_element_type=jnp.float32).astype(half)
        back = jnp.where(back_x == back_t + n * rest, 1.0, 0.0).astype(half)
        tails = jnp.dot(spec[s, main:, :], perm, preferred_element_type=jnp.float32).astype(half)
        wts[s, main:, :] = jnp.dot(back, tails, preferred_element_type=jnp.float32).astype(half)

    fine = lax.broadcasted_iota(jnp.int32, (KB, LANE), 1).astype(jnp.float32)
    lane = lax.broadcasted_iota(jnp.int32, (KB, LANE), 1)
    pieces = kchunk // KB
    steps = rows // ROW_STEP

    def row_count(r):
        a = lat[wi * rows + r]
        return 20 + 4 * jnp.minimum(a, NLAT - 1 - a)

    def basis_rows(c):
        for group, start in zip(groups, group_starts):
            if c in group:
                real = start + group.index(c) * kchunk
                return real, real + len(group) * kchunk

    group_starts = []
    for group in groups:
        group_starts.append(2 * kchunk * sum(len(g) for g in groups[: len(group_starts)]))

    def make_basis(c, unit):
        real0, imag0 = basis_rows(c)
        k0 = unit // steps * KB
        r0 = unit % steps * ROW_STEP
        m = waves[c * kchunk + k0 : c * kchunk + k0 + KB, :]
        counts = [row_count(r0 + i) for i in range(ROW_STEP)]
        each = jnp.full((KB, LANE), counts[0].astype(jnp.float32), jnp.float32)
        for i in range(1, ROW_STEP):
            each = jnp.where(lane == i, counts[i].astype(jnp.float32), each)
        stride_cos, stride_sin = trig(m * LANE, each, 1.0 / each)
        for i in range(ROW_STEP):
            r = r0 + i
            highest = jnp.minimum(wave_count - 1, lax.shift_right_logical(counts[i] - 1, 1)).astype(jnp.float32)
            count = jnp.full((KB, LANE), counts[i].astype(jnp.float32), jnp.float32)
            factor = jnp.where((m >= 0.0) & (m <= highest), jnp.where(m == 0.0, 1.0, 2.0), 0.0)
            sc = jnp.broadcast_to(stride_cos[:, i : i + 1], (KB, LANE))
            ss = jnp.broadcast_to(stride_sin[:, i : i + 1], (KB, LANE))
            c0, s0 = trig(m * fine, count, 1.0 / count)
            c0 = c0 * factor
            s0 = -(s0 * factor)
            c1 = c0 * sc + s0 * ss
            s1 = s0 * sc - c0 * ss
            twice = sc + sc
            for b in range(blocks):
                basis[r, b, real0 + k0 : real0 + k0 + KB, :] = c0.astype(half)
                basis[r, b, imag0 + k0 : imag0 + k0 + KB, :] = s0.astype(half)
                if b + 1 < blocks:
                    c0, c1 = c1, twice * c1 - c0
                    s0, s1 = s1, twice * s1 - s0

    cols = lax.broadcasted_iota(jnp.int32, (1, main), 1)
    tcols = lax.broadcasted_iota(jnp.int32, (1, LANE), 1)

    def fourier(c):
        lo, hi = bounds[c]
        for s in range(lo, hi):
            border = wave_count - wp[wi * slots + s]
            fold_rows = jnp.concatenate([cols, main + tcols - s % per_tile * rest], axis=1)
            low = jnp.where(fold_rows < border, 1.0, 0.0).astype(half)
            values = jnp.concatenate([
                leg[:, s].reshape(qtot, main),
                tail[:, s // per_tile].reshape(qtot, LANE),
            ], axis=1)
            picked = values * low
            f = jnp.dot(
                jnp.concatenate([picked, values - picked], axis=0), wts[s],
                preferred_element_type=jnp.float32,
            )
            for h in range(HALVES):
                stage[pl.ds(h * PACK + s - lo, qtot, stride=SIDE), :] = f[h * qtot : (h + 1) * qtot]
        snd[c] = stage[...].astype(half).reshape(snd.shape[1:])
        for k in order:
            exchange(c, k).start()
        mine = stage[pl.ds(pl.multiple_of(wi * rows * SIDE, rows * SIDE), rows * SIDE), :]
        rcv[c, wi] = mine.astype(half).reshape(rcv.shape[2:])

    def landed(c):
        for k in order:
            exchange(c, k).wait_recv()

    lanes = lax.broadcasted_iota(jnp.int32, (layers, COLS), 1)

    def synthesis(g):
        group = groups[g]
        for c in group:
            landed(c)
        depth = 2 * kchunk * len(group)

        def body(r, carry):
            v = jnp.concatenate([rcv[c, :, r].reshape(kchunk, items) for c in group], axis=0)
            vt = v.T
            lhs = jnp.concatenate([vt[:layers], vt[layers:]], axis=1)
            count = row_count(r)
            for n0 in range(0, full, COLS):
                n1 = min(full, n0 + COLS)
                rhs = jnp.concatenate([
                    basis[r, b, group_starts[g] : group_starts[g] + depth, :]
                    for b in range(n0 // LANE, n1 // LANE)
                ], axis=1)
                value = jnp.dot(lhs, rhs, preferred_element_type=jnp.float32)
                if g:
                    value = part[r, :, n0:n1] + value
                if g + 1 < len(groups):
                    part[r, :, n0:n1] = value
                else:
                    value = jnp.where(lanes[:, : n1 - n0] + n0 < count, value, 0.0)
                    stop = min(width, n1)
                    out_ref[r, :, n0:stop] = value[:, : stop - n0].astype(half)
            return carry

        lax.fori_loop(0, rows, body, 0, unroll=True)

    units = [(c, unit) for c in range(chunks) for unit in range(pieces * steps)]
    pace = -(-slots // len(units))
    done = {"weighed": 0, "made": 0}

    def prepare(upto):
        while done["weighed"] < min(slots, upto):
            weigh(done["weighed"])
            done["weighed"] += 1

    def work(upto):
        while done["made"] < min(len(units), upto):
            prepare(done["weighed"] + pace)
            make_basis(*units[done["made"]])
            done["made"] += 1

    spec_copy.wait()
    polls = sorted(((k, c) for k in range(nl - 1) for c in range(chunks)), key=lambda p: (p[0] + p[1], p[0]))
    shown = 0
    for k, c in polls:
        arrive(k, c)
        if k == 0 and ahead < chunks:
            send(0, ahead)
            ahead += 1
        if k == nl - 2:
            prepare(bounds[c][1])
            fourier(c)
            while shown < len(groups) and groups[shown][-1] + 3 <= c:
                work(len(units) // chunks * (groups[shown][-1] + 1))
                synthesis(shown)
                shown += 1
        work(done["made"] + 1)
    work(len(units))
    while shown < len(groups):
        synthesis(shown)
        shown += 1

    for c in range(chunks):
        for k in range(nl - 1):
            for way in range(2):
                going, block = sends(way, k)

                @pl.when(going)
                def _():
                    for hop in hops(way, k, c, block):
                        hop.wait_send()

        for k in order:
            exchange(c, k).wait_send()


def on_device(spectral, legendre, wave_pair, lat_slot):
    slots, fold, items = spectral.shape
    wave_count = fold - 1
    nw = lax.axis_size("wav")
    nl = lax.axis_size("lev")
    rows = lat_slot.shape[0] // nw
    layers = items // 2
    width = 2 * NLAT + 16
    full = -(-width // LANE) * LANE
    main = fold // LANE * LANE
    per_tile = LANE // (fold - main)
    bounds = chunk_plan(slots, per_tile)
    chunks = len(bounds)
    groups = group_plan(chunks)
    tiles = -(-slots // per_tile)
    leg_t = jnp.transpose(legendre, (0, 2, 1))
    lrows = leg_t.shape[1]
    kchunk = nw * SIDE

    hbm = pl.BlockSpec(memory_space=pl.ANY)
    dma = pltpu.SemaphoreType.DMA
    vmem = pltpu.VMEM
    half = jnp.bfloat16
    place = functools.partial(pltpu.with_memory_space_constraint, memory_space=pltpu.HBM)
    return pl.pallas_call(
        functools.partial(kernel, nw, nl, slots, wave_count, bounds, groups, per_tile),
        out_shape=vmem((rows, layers, width), half),
        in_specs=[hbm, hbm, hbm, hbm],
        out_specs=pl.BlockSpec(memory_space=vmem),
        scratch_shapes=[
            pltpu.SMEM(wave_pair.shape, jnp.int32),
            pltpu.SMEM(lat_slot.shape, jnp.int32),
            vmem((slots, fold, items), half),
            vmem((slots, lrows, fold), half),
            vmem((nl, slots, lrows, main), half),
            vmem((nl, tiles, lrows, LANE), half),
            vmem((slots, main + LANE, items), half),
            vmem((chunks * kchunk, LANE), jnp.float32),
            vmem((nw * rows * SIDE, items), jnp.float32),
            vmem((chunks, nw, rows, SIDE, items), half),
            vmem((chunks, nw, rows, SIDE, items), half),
            vmem((rows, full // LANE, 2 * chunks * kchunk, LANE), half),
            vmem((rows, layers, full), jnp.float32),
            dma((5,)),
            dma((2, nl - 1, chunks, 2)),
            dma((2, nl - 1, chunks, 2)),
            dma((chunks, nw)),
            dma((chunks, nw)),
        ],
        compiler_params=pltpu.CompilerParams(collective_id=0, has_side_effects=True, vmem_limit_bytes=52 << 20),
    )(place(wave_pair), place(lat_slot), place(spectral), place(leg_t))


def solution(mesh):
    return jax.shard_map(
        on_device,
        mesh=mesh,
        in_specs=(P("wav", None, "lev"), P("wav", None, "lev"), P(), P()),
        out_specs=P("wav", "lev", None),
        check_vma=False,
    )
```

```python
import functools
import math

import jax
import jax.numpy as jnp
from jax import lax
from jax.experimental import pallas as pl
from jax.experimental.pallas import tpu as pltpu
from jax.sharding import PartitionSpec as P

NLAT = 800
LANE = 128
PACK = 4
HALVES = 2
SIDE = HALVES * PACK
KB = 64
ROW_STEP = 4
COLS = 256


def half_turn(x):
    u = x * math.pi
    v = u * u
    s = -2.5052108385441720e-08
    for coef in (2.7557319223985893e-06, -1.9841269841269841e-04, 8.3333333333333333e-03, -1.6666666666666667e-01, 1.0):
        s = s * v + coef
    s = s * u
    c = -2.7557319223985888e-07
    for coef in (2.4801587301587302e-05, -1.3888888888888889e-03, 4.1666666666666667e-02, -0.5, 1.0):
        c = c * v + coef
    return 1.0 - 2.0 * s * s, 2.0 * s * c


def trig(prod, count, inv):
    r = prod - jnp.floor(prod * inv + 0.5) * count
    return half_turn(r * inv)


def chunk_plan(slots, per_tile):
    bounds = []
    for lo in range(0, slots, per_tile):
        hi = min(slots, lo + per_tile)
        for start in range(lo, hi, PACK):
            bounds.append((start, min(hi, start + PACK)))
    return bounds


def group_plan(chunks):
    paired = max(0, chunks - 3) // 2 * 2
    return [(c, c + 1) for c in range(0, paired, 2)] + [(c,) for c in range(paired, chunks)]


def exchange_order(nw):
    if nw & (nw - 1):
        return list(range(1, nw))
    return sorted(range(1, nw), key=lambda k: (-bin(k >> 1).count("1"), k))


def near(k):
    return bin(k >> 1).count("1") <= 1


def partner(wi, k, nw, sending):
    if nw & (nw - 1):
        return lax.rem(wi + (k if sending else nw - k), nw)
    other = wi
    bit = 1
    while bit < nw:
        if k & bit:
            other = other + bit * (1 - 2 * lax.rem(lax.div(wi, bit), 2))
        bit *= 2
    return other


def kernel(
    nw, nl, slots, wave_count, bounds, groups, per_tile,
    wp_hbm, lat_hbm, spec_hbm, leg_hbm, out_ref,
    wp, lat, spec, own, leg, tail, wts, waves, stage, snd, rcv, basis, part,
    loc_sem, ag_send, main_recv, tail_recv, aa_send, aa_recv, *gate,
):
    wi = lax.axis_index("wav")
    li = lax.axis_index("lev")
    chunks = len(bounds)
    rows, layers, width = out_ref.shape
    fold = spec.shape[1]
    main = leg.shape[3]
    rest = fold - main
    items = 2 * layers
    blocks = basis.shape[1]
    full = blocks * LANE
    kchunk = nw * SIDE
    qtot = nw * rows
    fmt = pl.DeviceIdType.MESH
    half = jnp.bfloat16

    copies = [
        pltpu.make_async_copy(src, dst, loc_sem.at[i])
        for i, (src, dst) in enumerate((
            (leg_hbm.at[:, :, pl.ds(0, main)], leg.at[li]),
            (leg_hbm, own),
            (wp_hbm, wp),
            (lat_hbm, lat),
            (spec_hbm, spec),
        ))
    ]
    for copy in copies:
        copy.start()
    leg_copy, own_copy, wp_copy, lat_copy, spec_copy = copies

    barrier = pltpu.get_barrier_semaphore()
    for step in (1, -1):
        @pl.when((li + step >= 0) & (li + step < nl))
        def _():
            pl.semaphore_signal(barrier, inc=1, device_id=(wi, li + step), device_id_type=fmt)
    order = exchange_order(nw)
    first = [k for k in order if near(k)] if gate else order
    for k in first:
        pl.semaphore_signal(barrier, inc=1, device_id=(partner(wi, k, nw, True), li), device_id_type=fmt)
    beside = jnp.where(li > 0, 1, 0) + jnp.where(li < nl - 1, 1, 0)
    pl.semaphore_wait(barrier, beside + len(first))
    direct = [k for k in first if not k & 1]

    def relay(stage):
        for k in direct:
            pl.semaphore_signal(gate[0].at[stage], inc=1, device_id=(partner(wi, k, nw, True), li), device_id_type=fmt)

    def everyone():
        for stage in range(len(direct) - 1 if gate else 0):
            pl.semaphore_wait(gate[0].at[stage], len(direct))
            if stage + 1 < len(direct) - 1:
                relay(stage + 1)

    def fresh(c):
        lo, hi = bounds[c]
        return [t for t in range(tail.shape[1]) if lo <= t * per_tile < hi]

    def hop(way, k, view, piece, recv):
        return pltpu.make_async_remote_copy(
            src_ref=view,
            dst_ref=view,
            send_sem=ag_send.at[way, k, piece],
            recv_sem=recv,
            device_id=(wi, li + 1 - 2 * way),
            device_id_type=fmt,
        )

    def main_hop(way, k, c, blocks):
        lo, hi = bounds[c]
        return hop(way, k, leg.at[blocks, pl.ds(lo, hi - lo)], 0, main_recv.at[k, c])

    def tail_hop(way, k, t, blocks):
        return hop(way, k, tail.at[blocks, t], 1, tail_recv.at[k, t])

    def hops(way, k, c, blocks, pieces=(0, 1)):
        chosen = [main_hop(way, k, c, blocks)] if 0 in pieces else []
        return chosen + ([tail_hop(way, k, t, blocks) for t in fresh(c)] if 1 in pieces else [])

    def sends(way, k):
        if way == 0:
            return (li - k >= 0) & (li + 1 < nl), jnp.maximum(li - k, 0)
        return (li + k < nl) & (li >= 1), jnp.minimum(li + k, nl - 1)

    def receives(way, k):
        if way == 0:
            return li - 1 - k >= 0, jnp.maximum(li - 1 - k, 0)
        return li + 1 + k < nl, jnp.minimum(li + 1 + k, nl - 1)

    def send(k, c, pieces=(0, 1)):
        for way in range(2):
            going, block = sends(way, k)

            @pl.when(going)
            def _():
                for hop in hops(way, k, c, block, pieces):
                    hop.start()

    def arrive(k, c):
        from_low, _ = receives(0, k)
        from_high, _ = receives(1, k)
        for come, number in ((from_low & from_high, 2), (from_low != from_high, 1)):
            @pl.when(come)
            def _():
                for copy in hops(0, k, c, pl.ds(0, number)):
                    copy.wait_recv()

        if k + 1 < nl - 1:
            send(k + 1, c)

    def exchange(c, k):
        dest = partner(wi, k, nw, True)
        return pltpu.make_async_remote_copy(
            src_ref=snd.at[c * nw + dest],
            dst_ref=rcv.at[c, wi],
            send_sem=aa_send.at[0],
            recv_sem=aa_recv.at[c],
            device_id=(dest, li),
            device_id_type=fmt,
        )

    def exchanged(c, src, dst):
        return pltpu.make_async_remote_copy(
            src_ref=src,
            dst_ref=dst,
            send_sem=aa_send.at[0],
            recv_sem=aa_recv.at[c],
            device_id=(partner(wi, 1, nw, True), li),
            device_id_type=fmt,
        )

    leg_copy.wait()
    send(0, 0, (0,))
    own_copy.wait()
    place_t = lax.broadcasted_iota(jnp.int32, (rest, LANE), 0)
    place_x = lax.broadcasted_iota(jnp.int32, (rest, LANE), 1)
    for t in range(tail.shape[1]):
        total = jnp.zeros(tail.shape[2:], jnp.float32)
        for n in range(per_tile):
            s = t * per_tile + n
            if s < slots:
                place = jnp.where(place_x == place_t + n * rest, 1.0, 0.0).astype(half)
                total += jnp.dot(own[s, :, main:], place, preferred_element_type=jnp.float32)
        tail[li, t] = total.astype(half)
    send(0, 0, (1,))
    ahead = min(chunks, 3)
    for c in range(1, ahead):
        send(0, c)
    if gate:
        relay(0)

    waves[...] = jnp.full_like(waves, -1.0)
    wp_copy.wait()
    lat_copy.wait()

    def place_waves(src, carry):
        for c, (lo, hi) in enumerate(bounds):
            for s in range(lo, hi):
                p = wp[src * slots + s]
                for h in range(HALVES):
                    m = jnp.where(p < 0, -1, p if h == 0 else wave_count - 1 - p).astype(jnp.float32)
                    row = c * kchunk + src * SIDE + h * PACK + s - lo
                    waves[pl.ds(row, 1), :] = jnp.full((1, LANE), m, jnp.float32)
        return carry

    lax.fori_loop(0, nw, place_waves, 0)

    stage[...] = jnp.zeros_like(stage)
    out_i = lax.broadcasted_iota(jnp.int32, (items, items), 1)
    in_i = lax.broadcasted_iota(jnp.int32, (items, items), 0)
    perm = jnp.where(
        in_i == jnp.where(out_i < layers, 2 * out_i, 2 * (out_i - layers) + 1), 1.0, 0.0
    ).astype(half)
    back_x = lax.broadcasted_iota(jnp.int32, (LANE, rest), 0)
    back_t = lax.broadcasted_iota(jnp.int32, (LANE, rest), 1)

    def weigh(s):
        n = s % per_tile
        wts[s, :main, :] = jnp.dot(spec[s, :main, :], perm, preferred_element_type=jnp.float32).astype(half)
        back = jnp.where(back_x == back_t + n * rest, 1.0, 0.0).astype(half)
        tails = jnp.dot(spec[s, main:, :], perm, preferred_element_type=jnp.float32).astype(half)
        wts[s, main:, :] = jnp.dot(back, tails, preferred_element_type=jnp.float32).astype(half)

    fine = lax.broadcasted_iota(jnp.int32, (KB, LANE), 1).astype(jnp.float32)
    lane = lax.broadcasted_iota(jnp.int32, (KB, LANE), 1)
    pieces = kchunk // KB
    steps = rows // ROW_STEP

    def row_count(r):
        a = lat[wi * rows + r]
        return 20 + 4 * jnp.minimum(a, NLAT - 1 - a)

    def basis_rows(c):
        for group, start in zip(groups, group_starts):
            if c in group:
                real = start + group.index(c) * kchunk
                return real, real + len(group) * kchunk

    group_starts = []
    for group in groups:
        group_starts.append(2 * kchunk * sum(len(g) for g in groups[: len(group_starts)]))

    def make_basis(c, unit):
        real0, imag0 = basis_rows(c)
        k0 = unit // steps * KB
        r0 = unit % steps * ROW_STEP
        m = waves[c * kchunk + k0 : c * kchunk + k0 + KB, :]
        counts = [row_count(r0 + i) for i in range(ROW_STEP)]
        each = jnp.full((KB, LANE), counts[0].astype(jnp.float32), jnp.float32)
        for i in range(1, ROW_STEP):
            each = jnp.where(lane == i, counts[i].astype(jnp.float32), each)
        stride_cos, stride_sin = trig(m * LANE, each, 1.0 / each)
        for i in range(ROW_STEP):
            r = r0 + i
            highest = jnp.minimum(wave_count - 1, lax.shift_right_logical(counts[i] - 1, 1)).astype(jnp.float32)
            count = jnp.full((KB, LANE), counts[i].astype(jnp.float32), jnp.float32)
            factor = jnp.where((m >= 0.0) & (m <= highest), jnp.where(m == 0.0, 1.0, 2.0), 0.0)
            sc = jnp.broadcast_to(stride_cos[:, i : i + 1], (KB, LANE))
            ss = jnp.broadcast_to(stride_sin[:, i : i + 1], (KB, LANE))
            c0, s0 = trig(m * fine, count, 1.0 / count)
            c0 = c0 * factor
            s0 = -(s0 * factor)
            c1 = c0 * sc + s0 * ss
            s1 = s0 * sc - c0 * ss
            twice = sc + sc
            for b in range(blocks):
                basis[r, b, real0 + k0 : real0 + k0 + KB, :] = c0.astype(half)
                basis[r, b, imag0 + k0 : imag0 + k0 + KB, :] = s0.astype(half)
                if b + 1 < blocks:
                    c0, c1 = c1, twice * c1 - c0
                    s0, s1 = s1, twice * s1 - s0

    cols = lax.broadcasted_iota(jnp.int32, (1, main), 1)
    tcols = lax.broadcasted_iota(jnp.int32, (1, LANE), 1)

    def fourier(c):
        lo, hi = bounds[c]
        for s in range(lo, hi):
            border = wave_count - wp[wi * slots + s]
            fold_rows = jnp.concatenate([cols, main + tcols - s % per_tile * rest], axis=1)
            low = jnp.where(fold_rows < border, 1.0, 0.0).astype(half)
            values = jnp.concatenate([
                leg[:, s].reshape(qtot, main),
                tail[:, s // per_tile].reshape(qtot, LANE),
            ], axis=1)
            picked = values * low
            f = jnp.dot(
                jnp.concatenate([picked, values - picked], axis=0), wts[s],
                preferred_element_type=jnp.float32,
            )
            for h in range(HALVES):
                stage[pl.ds(h * PACK + s - lo, qtot, stride=SIDE), :] = f[h * qtot : (h + 1) * qtot]
        snd[c * nw : (c + 1) * nw] = stage[...].astype(half).reshape((nw,) + snd.shape[1:])
        for k in order:
            exchange(c, k).start()
        mine = stage[pl.ds(pl.multiple_of(wi * rows * SIDE, rows * SIDE), rows * SIDE), :]
        rcv[c, wi] = mine.astype(half).reshape(rcv.shape[2:])

    def landed(c):
        others = pl.ds(0, nw - 1)
        exchanged(c, rcv.at[c, others], rcv.at[c, others]).wait_recv()

    lanes = lax.broadcasted_iota(jnp.int32, (layers, COLS), 1)

    def synthesis(g):
        group = groups[g]
        for c in group:
            landed(c)
        depth = 2 * kchunk * len(group)

        def body(r, carry):
            v = jnp.concatenate([rcv[c, :, r].reshape(kchunk, items) for c in group], axis=0)
            vt = v.T
            lhs = jnp.concatenate([vt[:layers], vt[layers:]], axis=1)
            count = row_count(r)
            for n0 in range(0, full, COLS):
                n1 = min(full, n0 + COLS)
                rhs = jnp.concatenate([
                    basis[r, b, group_starts[g] : group_starts[g] + depth, :]
                    for b in range(n0 // LANE, n1 // LANE)
                ], axis=1)
                value = jnp.dot(lhs, rhs, preferred_element_type=jnp.float32)
                if g:
                    value = part[r, :, n0:n1] + value
                if g + 1 < len(groups):
                    part[r, :, n0:n1] = value
                else:
                    value = jnp.where(lanes[:, : n1 - n0] + n0 < count, value, 0.0)
                    stop = min(width, n1)
                    out_ref[r, :, n0:stop] = value[:, : stop - n0].astype(half)
            return carry

        lax.fori_loop(0, rows, body, 0, unroll=True)

    units = [(c, unit) for c in range(chunks) for unit in range(pieces * steps)]
    pace = -(-slots // len(units))
    done = {"weighed": 0, "made": 0}

    def prepare(upto):
        while done["weighed"] < min(slots, upto):
            weigh(done["weighed"])
            done["weighed"] += 1

    def work(upto):
        while done["made"] < min(len(units), upto):
            prepare(done["weighed"] + pace)
            make_basis(*units[done["made"]])
            done["made"] += 1

    spec_copy.wait()
    polls = sorted(((k, c) for k in range(nl - 1) for c in range(chunks)), key=lambda p: (p[0] + p[1], p[0]))
    shown = 0
    for k, c in polls:
        arrive(k, c)
        if k == 0 and ahead < chunks:
            send(0, ahead)
            ahead += 1
        if k == nl - 2:
            prepare(bounds[c][1])
            if c == 0:
                everyone()
            fourier(c)
            while shown < len(groups) and groups[shown][-1] + 3 <= c:
                work(len(units) // chunks * (groups[shown][-1] + 1))
                synthesis(shown)
                shown += 1
        work(done["made"] + 1)
    work(len(units))
    while shown < len(groups):
        synthesis(shown)
        shown += 1

    for k in range(nl - 1):
        for way in range(2):
            going, block = sends(way, k)

            @pl.when(going)
            def _():
                hop(way, k, leg.at[block], 0, main_recv.at[k, 0]).wait_send()
                hop(way, k, tail.at[block], 1, tail_recv.at[k, 0]).wait_send()

    sent = snd.at[pl.ds(0, chunks * (nw - 1))]
    exchanged(0, sent, sent).wait_send()


def on_device(spectral, legendre, wave_pair, lat_slot):
    slots, fold, items = spectral.shape
    wave_count = fold - 1
    nw = lax.axis_size("wav")
    nl = lax.axis_size("lev")
    rows = lat_slot.shape[0] // nw
    layers = items // 2
    width = 2 * NLAT + 16
    full = -(-width // LANE) * LANE
    main = fold // LANE * LANE
    per_tile = LANE // (fold - main)
    bounds = chunk_plan(slots, per_tile)
    chunks = len(bounds)
    groups = group_plan(chunks)
    tiles = -(-slots // per_tile)
    leg_t = jnp.transpose(legendre, (0, 2, 1))
    lrows = leg_t.shape[1]
    kchunk = nw * SIDE

    bits = (nw >> 1).bit_length() - 1
    staged = nw & (nw - 1) == 0 and bits > 1
    gates = [pltpu.SemaphoreType.REGULAR((bits - 1,))] if staged else []

    hbm = pl.BlockSpec(memory_space=pl.ANY)
    dma = pltpu.SemaphoreType.DMA
    vmem = pltpu.VMEM
    half = jnp.bfloat16
    place = functools.partial(pltpu.with_memory_space_constraint, memory_space=pltpu.HBM)
    return pl.pallas_call(
        functools.partial(kernel, nw, nl, slots, wave_count, bounds, groups, per_tile),
        out_shape=vmem((rows, layers, width), half),
        in_specs=[hbm, hbm, hbm, hbm],
        out_specs=pl.BlockSpec(memory_space=vmem),
        scratch_shapes=[
            pltpu.SMEM(wave_pair.shape, jnp.int32),
            pltpu.SMEM(lat_slot.shape, jnp.int32),
            vmem((slots, fold, items), half),
            vmem((slots, lrows, fold), half),
            vmem((nl, slots, lrows, main), half),
            vmem((nl, tiles, lrows, LANE), half),
            vmem((slots, main + LANE, items), half),
            vmem((chunks * kchunk, LANE), jnp.float32),
            vmem((nw * rows * SIDE, items), jnp.float32),
            vmem((chunks * nw, rows, SIDE, items), half),
            vmem((chunks, nw, rows, SIDE, items), half),
            vmem((rows, full // LANE, 2 * chunks * kchunk, LANE), half),
            vmem((rows, layers, full), jnp.float32),
            dma((5,)),
            dma((2, nl - 1, 2)),
            dma((nl - 1, chunks)),
            dma((nl - 1, tiles)),
            dma((1,)),
            dma((chunks,)),
        ] + gates,
        compiler_params=pltpu.CompilerParams(collective_id=0, has_side_effects=True, vmem_limit_bytes=52 << 20),
    )(place(wave_pair), place(lat_slot), place(spectral), place(leg_t))


def solution(mesh):
    return jax.shard_map(
        on_device,
        mesh=mesh,
        in_specs=(P("wav", None, "lev"), P("wav", None, "lev"), P(), P()),
        out_specs=P("wav", "lev", None),
        check_vma=False,
    )
```

```python
import functools
import math

import jax
import jax.numpy as jnp
from jax import lax
from jax.experimental import pallas as pl
from jax.experimental.pallas import tpu as pltpu
from jax.sharding import PartitionSpec as P

NLAT = 800
LANE = 128
PACK = 4
HALVES = 2
SIDE = HALVES * PACK
KB = 64
ROW_STEP = 4
COLS = 256


def half_turn(x):
    u = x * math.pi
    v = u * u
    s = -2.5052108385441720e-08
    for coef in (2.7557319223985893e-06, -1.9841269841269841e-04, 8.3333333333333333e-03, -1.6666666666666667e-01, 1.0):
        s = s * v + coef
    s = s * u
    c = -2.7557319223985888e-07
    for coef in (2.4801587301587302e-05, -1.3888888888888889e-03, 4.1666666666666667e-02, -0.5, 1.0):
        c = c * v + coef
    return 1.0 - 2.0 * s * s, 2.0 * s * c


def trig(prod, count, inv):
    r = prod - jnp.floor(prod * inv + 0.5) * count
    return half_turn(r * inv)


def chunk_plan(slots, per_tile):
    bounds = []
    for lo in range(0, slots, per_tile):
        hi = min(slots, lo + per_tile)
        for start in range(lo, hi, PACK):
            bounds.append((start, min(hi, start + PACK)))
    return bounds


def group_plan(chunks):
    paired = max(0, chunks - 3) // 2 * 2
    return [(c, c + 1) for c in range(0, paired, 2)] + [(c,) for c in range(paired, chunks)]


def exchange_order(nw):
    if nw & (nw - 1):
        return list(range(1, nw))
    return sorted(range(1, nw), key=lambda k: (-bin(k >> 1).count("1"), k))


def near(k):
    return bin(k >> 1).count("1") <= 1


def partner(wi, k, nw, sending):
    if nw & (nw - 1):
        return lax.rem(wi + (k if sending else nw - k), nw)
    other = wi
    bit = 1
    while bit < nw:
        if k & bit:
            other = other + bit * (1 - 2 * lax.rem(lax.div(wi, bit), 2))
        bit *= 2
    return other


def kernel(
    nw, nl, slots, wave_count, bounds, groups, per_tile,
    wp_hbm, lat_hbm, spec_hbm, leg_hbm, out_ref,
    wp, lat, spec, own, leg, tail, wts, waves, stage, snd, rcv, basis, part,
    loc_sem, ag_send, main_recv, tail_recv, aa_send, aa_recv, gate,
):
    wi = lax.axis_index("wav")
    li = lax.axis_index("lev")
    chunks = len(bounds)
    rows, layers, width = out_ref.shape
    fold = spec.shape[1]
    main = leg.shape[3]
    rest = fold - main
    items = 2 * layers
    blocks = basis.shape[1]
    full = blocks * LANE
    kchunk = nw * SIDE
    qtot = nw * rows
    fmt = pl.DeviceIdType.MESH
    half = jnp.bfloat16

    copies = [
        pltpu.make_async_copy(src, dst, loc_sem.at[i])
        for i, (src, dst) in enumerate((
            (leg_hbm.at[:, :, pl.ds(0, main)], leg.at[li]),
            (leg_hbm, own),
            (wp_hbm, wp),
            (lat_hbm, lat),
            (spec_hbm, spec),
        ))
    ]
    for copy in copies:
        copy.start()
    leg_copy, own_copy, wp_copy, lat_copy, spec_copy = copies

    barrier = pltpu.get_barrier_semaphore()
    order = exchange_order(nw)
    stages = gate.shape[0] - 2
    first = [k for k in order if near(k)] if stages else order
    direct = [k for k in first if not k & 1]

    def tell(sem, w, l):
        pl.semaphore_signal(sem, inc=1, device_id=(w, l), device_id_type=fmt)

    lower = jnp.where(li > 0, 1, 0)
    higher = 0
    for k in first:
        to, source = partner(wi, k, nw, True), partner(wi, k, nw, False)
        lower += jnp.where(source < wi, 1, 0)
        higher += jnp.where(to > wi, 1, 0) if nw & (nw - 1) == 0 else jnp.where(source > wi, 1, 0)

    @pl.when(li + 1 < nl)
    def _():
        tell(barrier, wi, li + 1)

    for k in first:
        to = partner(wi, k, nw, True)

        @pl.when(to > wi)
        def _():
            tell(barrier, to, li)

    @pl.when(lower > 0)
    def _():
        pl.semaphore_wait(barrier, lower)

    @pl.when(li > 0)
    def _():
        tell(gate.at[1], wi, li - 1)

    for k in first:
        to = partner(wi, k, nw, True)

        @pl.when(to < wi)
        def _():
            tell(gate.at[0], to, li)

    def relay(stage):
        for k in direct:
            tell(gate.at[2 + stage], partner(wi, k, nw, True), li)

    def everyone():
        for stage in range(stages):
            pl.semaphore_wait(gate.at[2 + stage], len(direct))
            if stage + 1 < stages:
                relay(stage + 1)

    def fresh(c):
        lo, hi = bounds[c]
        return [t for t in range(tail.shape[1]) if lo <= t * per_tile < hi]

    def hop(way, k, view, piece, recv):
        return pltpu.make_async_remote_copy(
            src_ref=view,
            dst_ref=view,
            send_sem=ag_send.at[way, k, piece],
            recv_sem=recv,
            device_id=(wi, li + 1 - 2 * way),
            device_id_type=fmt,
        )

    def main_hop(way, k, c, blocks):
        lo, hi = bounds[c]
        return hop(way, k, leg.at[blocks, pl.ds(lo, hi - lo)], 0, main_recv.at[k, c])

    def tail_hop(way, k, t, blocks):
        return hop(way, k, tail.at[blocks, t], 1, tail_recv.at[k, t])

    def hops(way, k, c, blocks, pieces=(0, 1)):
        chosen = [main_hop(way, k, c, blocks)] if 0 in pieces else []
        return chosen + ([tail_hop(way, k, t, blocks) for t in fresh(c)] if 1 in pieces else [])

    def sends(way, k):
        if way == 0:
            return (li - k >= 0) & (li + 1 < nl), jnp.maximum(li - k, 0)
        return (li + k < nl) & (li >= 1), jnp.minimum(li + k, nl - 1)

    def receives(way, k):
        if way == 0:
            return li - 1 - k >= 0, jnp.maximum(li - 1 - k, 0)
        return li + 1 + k < nl, jnp.minimum(li + 1 + k, nl - 1)

    def send(k, c, pieces=(0, 1), ways=(0, 1)):
        for way in ways:
            going, block = sends(way, k)

            @pl.when(going)
            def _():
                for hop in hops(way, k, c, block, pieces):
                    hop.start()

    def arrive(k, c):
        from_low, _ = receives(0, k)
        from_high, _ = receives(1, k)
        for come, number in ((from_low & from_high, 2), (from_low != from_high, 1)):
            @pl.when(come)
            def _():
                for copy in hops(0, k, c, pl.ds(0, number)):
                    copy.wait_recv()

        if k + 1 < nl - 1:
            send(k + 1, c)

    def exchange(c, k):
        dest = partner(wi, k, nw, True)
        return pltpu.make_async_remote_copy(
            src_ref=snd.at[c * nw + dest],
            dst_ref=rcv.at[c, wi],
            send_sem=aa_send.at[0],
            recv_sem=aa_recv.at[c],
            device_id=(dest, li),
            device_id_type=fmt,
        )

    def exchanged(c, src, dst):
        return pltpu.make_async_remote_copy(
            src_ref=src,
            dst_ref=dst,
            send_sem=aa_send.at[0],
            recv_sem=aa_recv.at[c],
            device_id=(partner(wi, 1, nw, True), li),
            device_id_type=fmt,
        )

    leg_copy.wait()
    send(0, 0, (0,), (1,))
    own_copy.wait()
    place_t = lax.broadcasted_iota(jnp.int32, (rest, LANE), 0)
    place_x = lax.broadcasted_iota(jnp.int32, (rest, LANE), 1)
    for t in range(tail.shape[1]):
        total = jnp.zeros(tail.shape[2:], jnp.float32)
        for n in range(per_tile):
            s = t * per_tile + n
            if s < slots:
                place = jnp.where(place_x == place_t + n * rest, 1.0, 0.0).astype(half)
                total += jnp.dot(own[s, :, main:], place, preferred_element_type=jnp.float32)
        tail[li, t] = total.astype(half)
    send(0, 0, (1,), (1,))
    ahead = min(chunks, 3)
    for c in range(1, ahead):
        send(0, c, ways=(1,))

    @pl.when(li + 1 < nl)
    def _():
        pl.semaphore_wait(gate.at[1], 1)

    for c in range(ahead):
        send(0, c, ways=(0,))

    waves[...] = jnp.full_like(waves, -1.0)
    wp_copy.wait()
    lat_copy.wait()

    def place_waves(src, carry):
        for c, (lo, hi) in enumerate(bounds):
            for s in range(lo, hi):
                p = wp[src * slots + s]
                for h in range(HALVES):
                    m = jnp.where(p < 0, -1, p if h == 0 else wave_count - 1 - p).astype(jnp.float32)
                    row = c * kchunk + src * SIDE + h * PACK + s - lo
                    waves[pl.ds(row, 1), :] = jnp.full((1, LANE), m, jnp.float32)
        return carry

    lax.fori_loop(0, nw, place_waves, 0)
    @pl.when(higher > 0)
    def _():
        pl.semaphore_wait(gate.at[0], higher)

    if stages:
        relay(0)

    stage[...] = jnp.zeros_like(stage)
    out_i = lax.broadcasted_iota(jnp.int32, (items, items), 1)
    in_i = lax.broadcasted_iota(jnp.int32, (items, items), 0)
    perm = jnp.where(
        in_i == jnp.where(out_i < layers, 2 * out_i, 2 * (out_i - layers) + 1), 1.0, 0.0
    ).astype(half)
    back_x = lax.broadcasted_iota(jnp.int32, (LANE, rest), 0)
    back_t = lax.broadcasted_iota(jnp.int32, (LANE, rest), 1)

    def weigh(s):
        n = s % per_tile
        wts[s, :main, :] = jnp.dot(spec[s, :main, :], perm, preferred_element_type=jnp.float32).astype(half)
        back = jnp.where(back_x == back_t + n * rest, 1.0, 0.0).astype(half)
        tails = jnp.dot(spec[s, main:, :], perm, preferred_element_type=jnp.float32).astype(half)
        wts[s, main:, :] = jnp.dot(back, tails, preferred_element_type=jnp.float32).astype(half)

    fine = lax.broadcasted_iota(jnp.int32, (KB, LANE), 1).astype(jnp.float32)
    lane = lax.broadcasted_iota(jnp.int32, (KB, LANE), 1)
    pieces = kchunk // KB
    steps = rows // ROW_STEP

    def row_count(r):
        a = lat[wi * rows + r]
        return 20 + 4 * jnp.minimum(a, NLAT - 1 - a)

    def basis_rows(c):
        for group, start in zip(groups, group_starts):
            if c in group:
                real = start + group.index(c) * kchunk
                return real, real + len(group) * kchunk

    group_starts = []
    for group in groups:
        group_starts.append(2 * kchunk * sum(len(g) for g in groups[: len(group_starts)]))

    def make_basis(c, unit):
        real0, imag0 = basis_rows(c)
        k0 = unit // steps * KB
        r0 = unit % steps * ROW_STEP
        m = waves[c * kchunk + k0 : c * kchunk + k0 + KB, :]
        counts = [row_count(r0 + i) for i in range(ROW_STEP)]
        each = jnp.full((KB, LANE), counts[0].astype(jnp.float32), jnp.float32)
        for i in range(1, ROW_STEP):
            each = jnp.where(lane == i, counts[i].astype(jnp.float32), each)
        stride_cos, stride_sin = trig(m * LANE, each, 1.0 / each)
        for i in range(ROW_STEP):
            r = r0 + i
            highest = jnp.minimum(wave_count - 1, lax.shift_right_logical(counts[i] - 1, 1)).astype(jnp.float32)
            count = jnp.full((KB, LANE), counts[i].astype(jnp.float32), jnp.float32)
            factor = jnp.where((m >= 0.0) & (m <= highest), jnp.where(m == 0.0, 1.0, 2.0), 0.0)
            sc = jnp.broadcast_to(stride_cos[:, i : i + 1], (KB, LANE))
            ss = jnp.broadcast_to(stride_sin[:, i : i + 1], (KB, LANE))
            c0, s0 = trig(m * fine, count, 1.0 / count)
            c0 = c0 * factor
            s0 = -(s0 * factor)
            c1 = c0 * sc + s0 * ss
            s1 = s0 * sc - c0 * ss
            twice = sc + sc
            for b in range(blocks):
                basis[r, b, real0 + k0 : real0 + k0 + KB, :] = c0.astype(half)
                basis[r, b, imag0 + k0 : imag0 + k0 + KB, :] = s0.astype(half)
                if b + 1 < blocks:
                    c0, c1 = c1, twice * c1 - c0
                    s0, s1 = s1, twice * s1 - s0

    cols = lax.broadcasted_iota(jnp.int32, (1, main), 1)
    tcols = lax.broadcasted_iota(jnp.int32, (1, LANE), 1)

    def fourier(c):
        lo, hi = bounds[c]
        for s in range(lo, hi):
            border = wave_count - wp[wi * slots + s]
            fold_rows = jnp.concatenate([cols, main + tcols - s % per_tile * rest], axis=1)
            low = jnp.where(fold_rows < border, 1.0, 0.0).astype(half)
            values = jnp.concatenate([
                leg[:, s].reshape(qtot, main),
                tail[:, s // per_tile].reshape(qtot, LANE),
            ], axis=1)
            picked = values * low
            f = jnp.dot(
                jnp.concatenate([picked, values - picked], axis=0), wts[s],
                preferred_element_type=jnp.float32,
            )
            for h in range(HALVES):
                stage[pl.ds(h * PACK + s - lo, qtot, stride=SIDE), :] = f[h * qtot : (h + 1) * qtot]
        snd[c * nw : (c + 1) * nw] = stage[...].astype(half).reshape((nw,) + snd.shape[1:])
        for k in order:
            exchange(c, k).start()
        mine = stage[pl.ds(pl.multiple_of(wi * rows * SIDE, rows * SIDE), rows * SIDE), :]
        rcv[c, wi] = mine.astype(half).reshape(rcv.shape[2:])

    def landed(c):
        others = pl.ds(0, nw - 1)
        exchanged(c, rcv.at[c, others], rcv.at[c, others]).wait_recv()

    lanes = lax.broadcasted_iota(jnp.int32, (layers, COLS), 1)

    def synthesis(g):
        group = groups[g]
        for c in group:
            landed(c)
        depth = 2 * kchunk * len(group)

        def body(r, carry):
            v = jnp.concatenate([rcv[c, :, r].reshape(kchunk, items) for c in group], axis=0)
            vt = v.T
            lhs = jnp.concatenate([vt[:layers], vt[layers:]], axis=1)
            count = row_count(r)
            for n0 in range(0, full, COLS):
                n1 = min(full, n0 + COLS)
                rhs = jnp.concatenate([
                    basis[r, b, group_starts[g] : group_starts[g] + depth, :]
                    for b in range(n0 // LANE, n1 // LANE)
                ], axis=1)
                value = jnp.dot(lhs, rhs, preferred_element_type=jnp.float32)
                if g:
                    value = part[r, :, n0:n1] + value
                if g + 1 < len(groups):
                    part[r, :, n0:n1] = value
                else:
                    value = jnp.where(lanes[:, : n1 - n0] + n0 < count, value, 0.0)
                    stop = min(width, n1)
                    out_ref[r, :, n0:stop] = value[:, : stop - n0].astype(half)
            return carry

        lax.fori_loop(0, rows, body, 0, unroll=True)

    units = [(c, unit) for c in range(chunks) for unit in range(pieces * steps)]
    pace = -(-slots // len(units))
    done = {"weighed": 0, "made": 0}

    def prepare(upto):
        while done["weighed"] < min(slots, upto):
            weigh(done["weighed"])
            done["weighed"] += 1

    def work(upto):
        while done["made"] < min(len(units), upto):
            prepare(done["weighed"] + pace)
            make_basis(*units[done["made"]])
            done["made"] += 1

    spec_copy.wait()
    polls = sorted(((k, c) for k in range(nl - 1) for c in range(chunks)), key=lambda p: (1.5 * p[0] + p[1], p[0]))
    shown = 0
    for k, c in polls:
        arrive(k, c)
        if k == 0 and ahead < chunks:
            send(0, ahead)
            ahead += 1
        if k == nl - 2:
            prepare(bounds[c][1])
            if c == 0:
                everyone()
            fourier(c)
            while shown < len(groups) and groups[shown][-1] + 3 <= c:
                work(len(units) // chunks * (groups[shown][-1] + 1))
                synthesis(shown)
                shown += 1
        work(done["made"] + 1)
    work(len(units))
    while shown < len(groups):
        synthesis(shown)
        shown += 1

    for k in range(nl - 1):
        for way in range(2):
            going, block = sends(way, k)

            @pl.when(going)
            def _():
                hop(way, k, leg.at[block], 0, main_recv.at[k, 0]).wait_send()
                hop(way, k, tail.at[block], 1, tail_recv.at[k, 0]).wait_send()

    sent = snd.at[pl.ds(0, chunks * (nw - 1))]
    exchanged(0, sent, sent).wait_send()


def on_device(spectral, legendre, wave_pair, lat_slot):
    slots, fold, items = spectral.shape
    wave_count = fold - 1
    nw = lax.axis_size("wav")
    nl = lax.axis_size("lev")
    rows = lat_slot.shape[0] // nw
    layers = items // 2
    width = 2 * NLAT + 16
    full = -(-width // LANE) * LANE
    main = fold // LANE * LANE
    per_tile = LANE // (fold - main)
    bounds = chunk_plan(slots, per_tile)
    chunks = len(bounds)
    groups = group_plan(chunks)
    tiles = -(-slots // per_tile)
    leg_t = jnp.transpose(legendre, (0, 2, 1))
    lrows = leg_t.shape[1]
    kchunk = nw * SIDE

    bits = (nw >> 1).bit_length() - 1
    stages = max(0, bits - 1) if nw & (nw - 1) == 0 else 0

    hbm = pl.BlockSpec(memory_space=pl.ANY)
    dma = pltpu.SemaphoreType.DMA
    vmem = pltpu.VMEM
    half = jnp.bfloat16
    place = functools.partial(pltpu.with_memory_space_constraint, memory_space=pltpu.HBM)
    return pl.pallas_call(
        functools.partial(kernel, nw, nl, slots, wave_count, bounds, groups, per_tile),
        out_shape=vmem((rows, layers, width), half),
        in_specs=[hbm, hbm, hbm, hbm],
        out_specs=pl.BlockSpec(memory_space=vmem),
        scratch_shapes=[
            pltpu.SMEM(wave_pair.shape, jnp.int32),
            pltpu.SMEM(lat_slot.shape, jnp.int32),
            vmem((slots, fold, items), half),
            vmem((slots, lrows, fold), half),
            vmem((nl, slots, lrows, main), half),
            vmem((nl, tiles, lrows, LANE), half),
            vmem((slots, main + LANE, items), half),
            vmem((chunks * kchunk, LANE), jnp.float32),
            vmem((nw * rows * SIDE, items), jnp.float32),
            vmem((chunks * nw, rows, SIDE, items), half),
            vmem((chunks, nw, rows, SIDE, items), half),
            vmem((rows, full // LANE, 2 * chunks * kchunk, LANE), half),
            vmem((rows, layers, full), jnp.float32),
            dma((5,)),
            dma((2, nl - 1, 2)),
            dma((nl - 1, chunks)),
            dma((nl - 1, tiles)),
            dma((1,)),
            dma((chunks,)),
            pltpu.SemaphoreType.REGULAR((2 + stages,)),
        ],
        compiler_params=pltpu.CompilerParams(collective_id=0, has_side_effects=True, vmem_limit_bytes=52 << 20),
    )(place(wave_pair), place(lat_slot), place(spectral), place(leg_t))


def solution(mesh):
    return jax.shard_map(
        on_device,
        mesh=mesh,
        in_specs=(P("wav", None, "lev"), P("wav", None, "lev"), P(), P()),
        out_specs=P("wav", "lev", None),
        check_vma=False,
    )
```

```python
import functools
import math

import jax
import jax.numpy as jnp
from jax import lax
from jax.experimental import pallas as pl
from jax.experimental.pallas import tpu as pltpu
from jax.sharding import PartitionSpec as P

NLAT = 800
LANE = 128
PACK = 4
HALVES = 2
SIDE = HALVES * PACK
KB = 64
ROW_STEP = 4
COLS = 256


def half_turn(x):
    u = x * math.pi
    v = u * u
    s = -2.5052108385441720e-08
    for coef in (2.7557319223985893e-06, -1.9841269841269841e-04, 8.3333333333333333e-03, -1.6666666666666667e-01, 1.0):
        s = s * v + coef
    s = s * u
    c = -2.7557319223985888e-07
    for coef in (2.4801587301587302e-05, -1.3888888888888889e-03, 4.1666666666666667e-02, -0.5, 1.0):
        c = c * v + coef
    return 1.0 - 2.0 * s * s, 2.0 * s * c


def trig(prod, count, inv):
    r = prod - jnp.floor(prod * inv + 0.5) * count
    return half_turn(r * inv)


def chunk_plan(slots, per_tile):
    bounds = []
    for lo in range(0, slots, per_tile):
        hi = min(slots, lo + per_tile)
        for start in range(lo, hi, PACK):
            bounds.append((start, min(hi, start + PACK)))
    return bounds


def group_plan(chunks):
    paired = max(0, chunks - 3) // 2 * 2
    return [(c, c + 1) for c in range(0, paired, 2)] + [(c,) for c in range(paired, chunks)]


def exchange_order(nw):
    if nw & (nw - 1):
        return list(range(1, nw))
    return sorted(range(1, nw), key=lambda k: (-bin(k >> 1).count("1"), k))


def near(k):
    return bin(k >> 1).count("1") <= 1


def partner(wi, k, nw, sending):
    if nw & (nw - 1):
        return lax.rem(wi + (k if sending else nw - k), nw)
    other = wi
    bit = 1
    while bit < nw:
        if k & bit:
            other = other + bit * (1 - 2 * lax.rem(lax.div(wi, bit), 2))
        bit *= 2
    return other


def kernel(
    nw, nl, slots, wave_count, bounds, groups, per_tile,
    wp_hbm, lat_hbm, spec_hbm, leg_hbm, part, late, got,
    wp, lat, spec, own, leg, tail, wts, waves, stage, snd, rcv, basis,
    loc_sem, ag_send, main_recv, tail_recv, aa_send, aa_recv, gate,
):
    wi = lax.axis_index("wav")
    li = lax.axis_index("lev")
    chunks = len(bounds)
    rows, layers, full = part.shape
    fold = spec.shape[1]
    main = leg.shape[3]
    rest = fold - main
    items = 2 * layers
    blocks = full // LANE
    kchunk = nw * SIDE
    qtot = nw * rows
    fmt = pl.DeviceIdType.MESH
    half = jnp.bfloat16

    copies = [
        pltpu.make_async_copy(src, dst, loc_sem.at[i])
        for i, (src, dst) in enumerate((
            (leg_hbm.at[:, :, pl.ds(0, main)], leg.at[li]),
            (leg_hbm, own),
            (wp_hbm, wp),
            (lat_hbm, lat),
            (spec_hbm, spec),
        ))
    ]
    for copy in copies:
        copy.start()
    leg_copy, own_copy, wp_copy, lat_copy, spec_copy = copies

    barrier = pltpu.get_barrier_semaphore()
    order = exchange_order(nw)
    stages = gate.shape[0] - 2
    first = [k for k in order if near(k)] if stages else order
    direct = [k for k in first if not k & 1]

    def tell(sem, w, l):
        pl.semaphore_signal(sem, inc=1, device_id=(w, l), device_id_type=fmt)

    lower = jnp.where(li > 0, 1, 0)
    higher = 0
    for k in first:
        to, source = partner(wi, k, nw, True), partner(wi, k, nw, False)
        lower += jnp.where(source < wi, 1, 0)
        higher += jnp.where(to > wi, 1, 0) if nw & (nw - 1) == 0 else jnp.where(source > wi, 1, 0)

    @pl.when(li + 1 < nl)
    def _():
        tell(barrier, wi, li + 1)

    for k in first:
        to = partner(wi, k, nw, True)

        @pl.when(to > wi)
        def _():
            tell(barrier, to, li)

    @pl.when(lower > 0)
    def _():
        pl.semaphore_wait(barrier, lower)

    @pl.when(li > 0)
    def _():
        tell(gate.at[1], wi, li - 1)

    for k in first:
        to = partner(wi, k, nw, True)

        @pl.when(to < wi)
        def _():
            tell(gate.at[0], to, li)

    def relay(stage):
        for k in direct:
            tell(gate.at[2 + stage], partner(wi, k, nw, True), li)

    def everyone():
        for stage in range(stages):
            pl.semaphore_wait(gate.at[2 + stage], len(direct))
            if stage + 1 < stages:
                relay(stage + 1)

    def fresh(c):
        lo, hi = bounds[c]
        return [t for t in range(tail.shape[1]) if lo <= t * per_tile < hi]

    def hop(way, k, view, piece, recv):
        return pltpu.make_async_remote_copy(
            src_ref=view,
            dst_ref=view,
            send_sem=ag_send.at[way, piece],
            recv_sem=recv,
            device_id=(wi, li + 1 - 2 * way),
            device_id_type=fmt,
        )

    def main_hop(way, k, c, blocks):
        lo, hi = bounds[c]
        return hop(way, k, leg.at[blocks, pl.ds(lo, hi - lo)], 0, main_recv.at[k, c])

    def tail_hop(way, k, t, blocks):
        return hop(way, k, tail.at[blocks, t], 1, tail_recv.at[k, t])

    def hops(way, k, c, blocks, pieces=(0, 1)):
        chosen = [main_hop(way, k, c, blocks)] if 0 in pieces else []
        return chosen + ([tail_hop(way, k, t, blocks) for t in fresh(c)] if 1 in pieces else [])

    def sends(way, k):
        if way == 0:
            return (li - k >= 0) & (li + 1 < nl), jnp.maximum(li - k, 0)
        return (li + k < nl) & (li >= 1), jnp.minimum(li + k, nl - 1)

    def receives(way, k):
        if way == 0:
            return li - 1 - k >= 0, jnp.maximum(li - 1 - k, 0)
        return li + 1 + k < nl, jnp.minimum(li + 1 + k, nl - 1)

    def send(k, c, pieces=(0, 1), ways=(0, 1)):
        for way in ways:
            going, block = sends(way, k)

            @pl.when(going)
            def _():
                for hop in hops(way, k, c, block, pieces):
                    hop.start()

    def arrive(k, c):
        from_low, _ = receives(0, k)
        from_high, _ = receives(1, k)
        for come, number in ((from_low & from_high, 2), (from_low != from_high, 1)):
            @pl.when(come)
            def _():
                for copy in hops(0, k, c, pl.ds(0, number)):
                    copy.wait_recv()

        if k + 1 < nl - 1:
            send(k + 1, c)

    def exchange(c, k):
        dest = partner(wi, k, nw, True)
        return pltpu.make_async_remote_copy(
            src_ref=snd.at[c * nw + dest],
            dst_ref=rcv.at[c, wi],
            send_sem=aa_send.at[0],
            recv_sem=aa_recv.at[c],
            device_id=(dest, li),
            device_id_type=fmt,
        )

    def exchanged(c, src, dst):
        return pltpu.make_async_remote_copy(
            src_ref=src,
            dst_ref=dst,
            send_sem=aa_send.at[0],
            recv_sem=aa_recv.at[c],
            device_id=(partner(wi, 1, nw, True), li),
            device_id_type=fmt,
        )

    leg_copy.wait()
    send(0, 0, (0,), (1,))
    own_copy.wait()
    place_t = lax.broadcasted_iota(jnp.int32, (rest, LANE), 0)
    place_x = lax.broadcasted_iota(jnp.int32, (rest, LANE), 1)
    for t in range(tail.shape[1]):
        total = jnp.zeros(tail.shape[2:], jnp.float32)
        for n in range(per_tile):
            s = t * per_tile + n
            if s < slots:
                place = jnp.where(place_x == place_t + n * rest, 1.0, 0.0).astype(half)
                total += jnp.dot(own[s, :, main:], place, preferred_element_type=jnp.float32)
        tail[li, t] = total.astype(half)
    send(0, 0, (1,), (1,))
    ahead = min(chunks, 3)
    for c in range(1, ahead):
        send(0, c, ways=(1,))

    @pl.when(li + 1 < nl)
    def _():
        pl.semaphore_wait(gate.at[1], 1)

    for c in range(ahead):
        send(0, c, ways=(0,))

    waves[...] = jnp.full_like(waves, -1.0)
    wp_copy.wait()
    lat_copy.wait()

    def place_waves(src, carry):
        for c, (lo, hi) in enumerate(bounds):
            for s in range(lo, hi):
                p = wp[src * slots + s]
                for h in range(HALVES):
                    m = jnp.where(p < 0, -1, p if h == 0 else wave_count - 1 - p).astype(jnp.float32)
                    row = c * kchunk + src * SIDE + h * PACK + s - lo
                    waves[pl.ds(row, 1), :] = jnp.full((1, LANE), m, jnp.float32)
        return carry

    lax.fori_loop(0, nw, place_waves, 0)
    @pl.when(higher > 0)
    def _():
        pl.semaphore_wait(gate.at[0], higher)

    if stages:
        relay(0)

    stage[...] = jnp.zeros_like(stage)
    out_i = lax.broadcasted_iota(jnp.int32, (items, items), 1)
    in_i = lax.broadcasted_iota(jnp.int32, (items, items), 0)
    perm = jnp.where(
        in_i == jnp.where(out_i < layers, 2 * out_i, 2 * (out_i - layers) + 1), 1.0, 0.0
    ).astype(half)
    back_x = lax.broadcasted_iota(jnp.int32, (LANE, rest), 0)
    back_t = lax.broadcasted_iota(jnp.int32, (LANE, rest), 1)

    def weigh(s):
        n = s % per_tile
        wts[s, :main, :] = jnp.dot(spec[s, :main, :], perm, preferred_element_type=jnp.float32).astype(half)
        back = jnp.where(back_x == back_t + n * rest, 1.0, 0.0).astype(half)
        tails = jnp.dot(spec[s, main:, :], perm, preferred_element_type=jnp.float32).astype(half)
        wts[s, main:, :] = jnp.dot(back, tails, preferred_element_type=jnp.float32).astype(half)

    fine = lax.broadcasted_iota(jnp.int32, (KB, LANE), 1).astype(jnp.float32)
    lane = lax.broadcasted_iota(jnp.int32, (KB, LANE), 1)
    pieces = kchunk // KB
    steps = rows // ROW_STEP

    def row_count(r):
        a = lat[wi * rows + r]
        return 20 + 4 * jnp.minimum(a, NLAT - 1 - a)

    def basis_rows(c):
        for group, start in zip(groups, group_starts):
            if c in group:
                real = start + group.index(c) * kchunk
                return real, real + len(group) * kchunk

    group_starts = []
    for group in groups:
        group_starts.append(2 * kchunk * sum(len(g) for g in groups[: len(group_starts)]))

    def make_basis(c, unit):
        real0, imag0 = basis_rows(c)
        k0 = unit // steps * KB
        r0 = unit % steps * ROW_STEP
        m = waves[c * kchunk + k0 : c * kchunk + k0 + KB, :]
        counts = [row_count(r0 + i) for i in range(ROW_STEP)]
        each = jnp.full((KB, LANE), counts[0].astype(jnp.float32), jnp.float32)
        for i in range(1, ROW_STEP):
            each = jnp.where(lane == i, counts[i].astype(jnp.float32), each)
        stride_cos, stride_sin = trig(m * LANE, each, 1.0 / each)
        for i in range(ROW_STEP):
            r = r0 + i
            highest = jnp.minimum(wave_count - 1, lax.shift_right_logical(counts[i] - 1, 1)).astype(jnp.float32)
            count = jnp.full((KB, LANE), counts[i].astype(jnp.float32), jnp.float32)
            factor = jnp.where((m >= 0.0) & (m <= highest), jnp.where(m == 0.0, 1.0, 2.0), 0.0)
            sc = jnp.broadcast_to(stride_cos[:, i : i + 1], (KB, LANE))
            ss = jnp.broadcast_to(stride_sin[:, i : i + 1], (KB, LANE))
            c0, s0 = trig(m * fine, count, 1.0 / count)
            c0 = c0 * factor
            s0 = -(s0 * factor)
            c1 = c0 * sc + s0 * ss
            s1 = s0 * sc - c0 * ss
            twice = sc + sc
            final = c in groups[-1]
            table = late if final else basis
            base = group_starts[-1] if final else 0
            for b in range(blocks):
                keep = lane + b * LANE < counts[i]
                cb, sb = (jnp.where(keep, c0, 0.0), jnp.where(keep, s0, 0.0)) if final else (c0, s0)
                table[r, b, real0 - base + k0 : real0 - base + k0 + KB, :] = cb.astype(half)
                table[r, b, imag0 - base + k0 : imag0 - base + k0 + KB, :] = sb.astype(half)
                if b + 1 < blocks:
                    c0, c1 = c1, twice * c1 - c0
                    s0, s1 = s1, twice * s1 - s0

    cols = lax.broadcasted_iota(jnp.int32, (1, main), 1)
    tcols = lax.broadcasted_iota(jnp.int32, (1, LANE), 1)

    def fourier(c):
        lo, hi = bounds[c]
        for s in range(lo, hi):
            border = wave_count - wp[wi * slots + s]
            fold_rows = jnp.concatenate([cols, main + tcols - s % per_tile * rest], axis=1)
            low = jnp.where(fold_rows < border, 1.0, 0.0).astype(half)
            values = jnp.concatenate([
                leg[:, s].reshape(qtot, main),
                tail[:, s // per_tile].reshape(qtot, LANE),
            ], axis=1)
            picked = values * low
            f = jnp.dot(
                jnp.concatenate([picked, values - picked], axis=0), wts[s],
                preferred_element_type=jnp.float32,
            )
            for h in range(HALVES):
                stage[pl.ds(h * PACK + s - lo, qtot, stride=SIDE), :] = f[h * qtot : (h + 1) * qtot]
        snd[c * nw : (c + 1) * nw] = stage[...].astype(half).reshape((nw,) + snd.shape[1:])
        for k in order:
            exchange(c, k).start()
        mine = stage[pl.ds(pl.multiple_of(wi * rows * SIDE, rows * SIDE), rows * SIDE), :]
        rcv[c, wi] = mine.astype(half).reshape(rcv.shape[2:])

    def landed(c):
        others = pl.ds(0, nw - 1)
        exchanged(c, rcv.at[c, others], rcv.at[c, others]).wait_recv()

    lanes = lax.broadcasted_iota(jnp.int32, (layers, COLS), 1)

    def synthesis(g):
        group = groups[g]
        for c in group:
            landed(c)
        depth = 2 * kchunk * len(group)

        def body(r, carry):
            v = jnp.concatenate([rcv[c, :, r].reshape(kchunk, items) for c in group], axis=0)
            vt = v.T
            lhs = jnp.concatenate([vt[:layers], vt[layers:]], axis=1)
            count = row_count(r)
            for n0 in range(0, full, COLS):
                n1 = min(full, n0 + COLS)
                rhs = jnp.concatenate([
                    basis[r, b, group_starts[g] : group_starts[g] + depth, :]
                    for b in range(n0 // LANE, n1 // LANE)
                ], axis=1)
                value = jnp.dot(lhs, rhs, preferred_element_type=jnp.float32)
                if g:
                    value = part[r, :, n0:n1] + value
                if g + 2 == len(groups):
                    value = jnp.where(lanes[:, : n1 - n0] + n0 < count, value, 0.0)
                part[r, :, n0:n1] = value
            return carry

        lax.fori_loop(0, rows, body, 0, unroll=True)

    units = [(c, unit) for c in range(chunks) for unit in range(pieces * steps)]
    pace = -(-slots // len(units))
    done = {"weighed": 0, "made": 0}

    def prepare(upto):
        while done["weighed"] < min(slots, upto):
            weigh(done["weighed"])
            done["weighed"] += 1

    def work(upto):
        while done["made"] < min(len(units), upto):
            prepare(done["weighed"] + pace)
            make_basis(*units[done["made"]])
            done["made"] += 1

    spec_copy.wait()
    polls = sorted(((k, c) for k in range(nl - 1) for c in range(chunks)), key=lambda p: (1.5 * p[0] + p[1], p[0]))
    shown = 0
    for k, c in polls:
        arrive(k, c)
        if k == 0 and ahead < chunks:
            send(0, ahead)
            ahead += 1
        if k == nl - 2:
            prepare(bounds[c][1])
            if c == 0:
                everyone()
            fourier(c)
            while shown < len(groups) and groups[shown][-1] + 3 <= c:
                work(len(units) // chunks * (groups[shown][-1] + 1))
                synthesis(shown)
                shown += 1
        work(done["made"] + 1)
    work(len(units))
    while shown < len(groups) - 1:
        synthesis(shown)
        shown += 1
    for n, c in enumerate(groups[-1]):
        landed(c)
        got[n] = rcv[c]

    for place in range(nl):
        for way, number in ((0, place + 1), (1, nl - place)):
            if number < nl:
                @pl.when(li == place)
                def _():
                    every = pl.ds(0, number)
                    hop(way, 0, leg.at[every], 0, main_recv.at[0, 0]).wait_send()
                    hop(way, 0, tail.at[every], 1, tail_recv.at[0, 0]).wait_send()

    sent = snd.at[pl.ds(0, chunks * (nw - 1))]
    exchanged(0, sent, sent).wait_send()


def finish(alone, part, late, got, out_hbm, rows_buf, out_sem):
    rows, layers, width = out_hbm.shape
    full = part.shape[2]
    items = got.shape[-1]
    depth = got.shape[1] * got.shape[3]
    for r in range(rows):
        v = jnp.concatenate([got[n, :, r].reshape(depth, items) for n in range(got.shape[0])], axis=0)
        vt = v.T
        lhs = jnp.concatenate([vt[:layers], vt[layers:]], axis=1)
        for n0 in range(0, full, COLS):
            n1 = min(full, n0 + COLS)
            rhs = jnp.concatenate([late[r, b] for b in range(n0 // LANE, n1 // LANE)], axis=1)
            value = jnp.dot(lhs, rhs, preferred_element_type=jnp.float32)
            if not alone:
                value = part[r, :, n0:n1] + value
            stop = min(width, n1)
            rows_buf[r, :, n0:stop] = value[:, : stop - n0].astype(jnp.bfloat16)
        pltpu.make_async_copy(rows_buf.at[r], out_hbm.at[r], out_sem.at[r]).start()
    for r in range(rows):
        pltpu.make_async_copy(rows_buf.at[r], out_hbm.at[r], out_sem.at[r]).wait()


def on_device(spectral, legendre, wave_pair, lat_slot):
    slots, fold, items = spectral.shape
    wave_count = fold - 1
    nw = lax.axis_size("wav")
    nl = lax.axis_size("lev")
    rows = lat_slot.shape[0] // nw
    layers = items // 2
    width = 2 * NLAT + 16
    full = -(-width // LANE) * LANE
    main = fold // LANE * LANE
    per_tile = LANE // (fold - main)
    bounds = chunk_plan(slots, per_tile)
    chunks = len(bounds)
    groups = group_plan(chunks)
    tiles = -(-slots // per_tile)
    leg_t = jnp.transpose(legendre, (0, 2, 1))
    lrows = leg_t.shape[1]
    kchunk = nw * SIDE

    bits = (nw >> 1).bit_length() - 1
    stages = max(0, bits - 1) if nw & (nw - 1) == 0 else 0

    hbm = pl.BlockSpec(memory_space=pl.ANY)
    dma = pltpu.SemaphoreType.DMA
    vmem = pltpu.VMEM
    half = jnp.bfloat16
    place = functools.partial(pltpu.with_memory_space_constraint, memory_space=pltpu.HBM)
    last = 2 * kchunk * len(groups[-1])
    handed = pl.pallas_call(
        functools.partial(kernel, nw, nl, slots, wave_count, bounds, groups, per_tile),
        out_shape=[
            vmem((rows, layers, full), jnp.float32),
            vmem((rows, full // LANE, last, LANE), half),
            vmem((len(groups[-1]), nw, rows, SIDE, items), half),
        ],
        in_specs=[hbm, hbm, hbm, hbm],
        out_specs=[pl.BlockSpec(memory_space=vmem)] * 3,
        scratch_shapes=[
            pltpu.SMEM(wave_pair.shape, jnp.int32),
            pltpu.SMEM(lat_slot.shape, jnp.int32),
            vmem((slots, fold, items), half),
            vmem((slots, lrows, fold), half),
            vmem((nl, slots, lrows, main), half),
            vmem((nl, tiles, lrows, LANE), half),
            vmem((slots, main + LANE, items), half),
            vmem((chunks * kchunk, LANE), jnp.float32),
            vmem((nw * rows * SIDE, items), jnp.float32),
            vmem((chunks * nw, rows, SIDE, items), half),
            vmem((chunks, nw, rows, SIDE, items), half),
            vmem((rows, full // LANE, 2 * chunks * kchunk - last, LANE), half),
            dma((5,)),
            dma((2, 2)),
            dma((nl - 1, chunks)),
            dma((nl - 1, tiles)),
            dma((1,)),
            dma((chunks,)),
            pltpu.SemaphoreType.REGULAR((2 + stages,)),
        ],
        compiler_params=pltpu.CompilerParams(collective_id=0, has_side_effects=True, vmem_limit_bytes=44 << 20),
    )(place(wave_pair), place(lat_slot), place(spectral), place(leg_t))
    return pl.pallas_call(
        functools.partial(finish, len(groups) == 1),
        out_shape=jax.ShapeDtypeStruct((rows, layers, width), half),
        in_specs=[pl.BlockSpec(memory_space=vmem)] * 3,
        out_specs=hbm,
        scratch_shapes=[vmem((rows, layers, width), half), dma((rows,))],
        compiler_params=pltpu.CompilerParams(vmem_limit_bytes=8 << 20),
    )(*handed)


def solution(mesh):
    return jax.shard_map(
        on_device,
        mesh=mesh,
        in_specs=(P("wav", None, "lev"), P("wav", None, "lev"), P(), P()),
        out_specs=P("wav", "lev", None),
        check_vma=False,
    )
```

```python
import functools
import math

import jax
import jax.numpy as jnp
from jax import lax
from jax.experimental import pallas as pl
from jax.experimental.pallas import tpu as pltpu
from jax.sharding import PartitionSpec as P

NLAT = 800
LANE = 128
PACK = 4
HALVES = 2
SIDE = HALVES * PACK
KB = 64
ROW_STEP = 4
COLS = 256


def half_turn(x):
    u = x * math.pi
    v = u * u
    s = -2.5052108385441720e-08
    for coef in (2.7557319223985893e-06, -1.9841269841269841e-04, 8.3333333333333333e-03, -1.6666666666666667e-01, 1.0):
        s = s * v + coef
    s = s * u
    c = -2.7557319223985888e-07
    for coef in (2.4801587301587302e-05, -1.3888888888888889e-03, 4.1666666666666667e-02, -0.5, 1.0):
        c = c * v + coef
    return 1.0 - 2.0 * s * s, 2.0 * s * c


def trig(prod, count, inv):
    r = prod - jnp.floor(prod * inv + 0.5) * count
    return half_turn(r * inv)


def chunk_plan(slots, per_tile):
    bounds = []
    for lo in range(0, slots, per_tile):
        hi = min(slots, lo + per_tile)
        for start in range(lo, hi, PACK):
            bounds.append((start, min(hi, start + PACK)))
    return bounds


def group_plan(chunks):
    paired = max(0, chunks - 3) // 2 * 2
    return [(c, c + 1) for c in range(0, paired, 2)] + [(c,) for c in range(paired, chunks)]


def exchange_order(nw):
    if nw & (nw - 1):
        return list(range(1, nw))
    return sorted(range(1, nw), key=lambda k: (-bin(k >> 1).count("1"), k))


def near(k):
    return bin(k >> 1).count("1") <= 1


def partner(wi, k, nw, sending):
    if nw & (nw - 1):
        return lax.rem(wi + (k if sending else nw - k), nw)
    other = wi
    bit = 1
    while bit < nw:
        if k & bit:
            other = other + bit * (1 - 2 * lax.rem(lax.div(wi, bit), 2))
        bit *= 2
    return other


def kernel(
    nw, nl, slots, wave_count, bounds, groups, per_tile,
    wp_hbm, lat_hbm, spec_hbm, leg_hbm, part, late, got,
    wp, lat, spec, own, leg, tail, wts, waves, stage, snd, rcv, basis,
    loc_sem, ag_send, main_recv, tail_recv, aa_send, aa_recv, gate,
):
    wi = lax.axis_index("wav")
    li = lax.axis_index("lev")
    chunks = len(bounds)
    rows, layers, full = part.shape
    fold = spec.shape[1]
    main = leg.shape[3]
    rest = fold - main
    items = 2 * layers
    blocks = full // LANE
    kchunk = nw * SIDE
    qtot = nw * rows
    fmt = pl.DeviceIdType.MESH
    half = jnp.bfloat16

    copies = [
        pltpu.make_async_copy(src, dst, loc_sem.at[i])
        for i, (src, dst) in enumerate((
            (leg_hbm.at[:, :, pl.ds(0, main)], leg.at[li]),
            (leg_hbm, own),
            (wp_hbm, wp),
            (lat_hbm, lat),
            (spec_hbm, spec),
        ))
    ]
    for copy in copies:
        copy.start()
    leg_copy, own_copy, wp_copy, lat_copy, spec_copy = copies

    barrier = pltpu.get_barrier_semaphore()
    order = exchange_order(nw)
    stages = gate.shape[0] - 2
    first = [k for k in order if near(k)] if stages else order
    direct = [k for k in first if not k & 1]

    def tell(sem, w, l):
        pl.semaphore_signal(sem, inc=1, device_id=(w, l), device_id_type=fmt)

    lower = jnp.where(li > 0, 1, 0)
    higher = 0
    for k in first:
        to, source = partner(wi, k, nw, True), partner(wi, k, nw, False)
        lower += jnp.where(source < wi, 1, 0)
        higher += jnp.where(to > wi, 1, 0) if nw & (nw - 1) == 0 else jnp.where(source > wi, 1, 0)

    @pl.when(li + 1 < nl)
    def _():
        tell(barrier, wi, li + 1)

    for k in first:
        to = partner(wi, k, nw, True)

        @pl.when(to > wi)
        def _():
            tell(barrier, to, li)

    @pl.when(lower > 0)
    def _():
        pl.semaphore_wait(barrier, lower)

    @pl.when(li > 0)
    def _():
        tell(gate.at[1], wi, li - 1)

    for k in first:
        to = partner(wi, k, nw, True)

        @pl.when(to < wi)
        def _():
            tell(gate.at[0], to, li)

    def relay(stage):
        for k in direct:
            tell(gate.at[2 + stage], partner(wi, k, nw, True), li)

    def everyone():
        for stage in range(stages):
            pl.semaphore_wait(gate.at[2 + stage], len(direct))
            if stage + 1 < stages:
                relay(stage + 1)

    def fresh(c):
        lo, hi = bounds[c]
        return [t for t in range(tail.shape[1]) if lo <= t * per_tile < hi]

    def hop(way, k, view, piece, recv):
        return pltpu.make_async_remote_copy(
            src_ref=view,
            dst_ref=view,
            send_sem=ag_send.at[way, piece],
            recv_sem=recv,
            device_id=(wi, li + 1 - 2 * way),
            device_id_type=fmt,
        )

    def main_hop(way, k, c, blocks):
        lo, hi = bounds[c]
        return hop(way, k, leg.at[blocks, pl.ds(lo, hi - lo)], 0, main_recv.at[k, c])

    def tail_hop(way, k, t, blocks):
        return hop(way, k, tail.at[blocks, t], 1, tail_recv.at[k, t])

    def hops(way, k, c, blocks, pieces=(0, 1)):
        chosen = [main_hop(way, k, c, blocks)] if 0 in pieces else []
        return chosen + ([tail_hop(way, k, t, blocks) for t in fresh(c)] if 1 in pieces else [])

    def sends(way, k):
        if way == 0:
            return (li - k >= 0) & (li + 1 < nl), jnp.maximum(li - k, 0)
        return (li + k < nl) & (li >= 1), jnp.minimum(li + k, nl - 1)

    def receives(way, k):
        if way == 0:
            return li - 1 - k >= 0, jnp.maximum(li - 1 - k, 0)
        return li + 1 + k < nl, jnp.minimum(li + 1 + k, nl - 1)

    def send(k, c, pieces=(0, 1), ways=(0, 1)):
        for way in ways:
            going, block = sends(way, k)

            @pl.when(going)
            def _():
                for hop in hops(way, k, c, block, pieces):
                    hop.start()

    def arrive(k, c):
        from_low, _ = receives(0, k)
        from_high, _ = receives(1, k)
        for come, number in ((from_low & from_high, 2), (from_low != from_high, 1)):
            @pl.when(come)
            def _():
                for copy in hops(0, k, c, pl.ds(0, number)):
                    copy.wait_recv()

        if k + 1 < nl - 1:
            send(k + 1, c)

    def exchange(c, k):
        dest = partner(wi, k, nw, True)
        return pltpu.make_async_remote_copy(
            src_ref=snd.at[c * nw + dest],
            dst_ref=rcv.at[c, wi],
            send_sem=aa_send.at[0],
            recv_sem=aa_recv.at[c],
            device_id=(dest, li),
            device_id_type=fmt,
        )

    def exchanged(c, src, dst):
        return pltpu.make_async_remote_copy(
            src_ref=src,
            dst_ref=dst,
            send_sem=aa_send.at[0],
            recv_sem=aa_recv.at[c],
            device_id=(partner(wi, 1, nw, True), li),
            device_id_type=fmt,
        )

    leg_copy.wait()
    send(0, 0, (0,), (1,))
    own_copy.wait()
    place_t = lax.broadcasted_iota(jnp.int32, (rest, LANE), 0)
    place_x = lax.broadcasted_iota(jnp.int32, (rest, LANE), 1)
    for t in range(tail.shape[1]):
        total = jnp.zeros(tail.shape[2:], jnp.float32)
        for n in range(per_tile):
            s = t * per_tile + n
            if s < slots:
                place = jnp.where(place_x == place_t + n * rest, 1.0, 0.0).astype(half)
                total += jnp.dot(own[s, :, main:], place, preferred_element_type=jnp.float32)
        tail[li, t] = total.astype(half)
    send(0, 0, (1,), (1,))
    ahead = min(chunks, 3)
    for c in range(1, ahead):
        send(0, c, ways=(1,))

    @pl.when(li + 1 < nl)
    def _():
        pl.semaphore_wait(gate.at[1], 1)

    for c in range(ahead):
        send(0, c, ways=(0,))

    waves[...] = jnp.full_like(waves, -1.0)
    wp_copy.wait()
    lat_copy.wait()

    def place_waves(src, carry):
        for c, (lo, hi) in enumerate(bounds):
            for s in range(lo, hi):
                p = wp[src * slots + s]
                for h in range(HALVES):
                    m = jnp.where(p < 0, -1, p if h == 0 else wave_count - 1 - p).astype(jnp.float32)
                    row = c * kchunk + src * SIDE + h * PACK + s - lo
                    waves[pl.ds(row, 1), :] = jnp.full((1, LANE), m, jnp.float32)
        return carry

    lax.fori_loop(0, nw, place_waves, 0)
    @pl.when(higher > 0)
    def _():
        pl.semaphore_wait(gate.at[0], higher)

    if stages:
        relay(0)

    stage[...] = jnp.zeros_like(stage)
    out_i = lax.broadcasted_iota(jnp.int32, (items, items), 1)
    in_i = lax.broadcasted_iota(jnp.int32, (items, items), 0)
    perm = jnp.where(
        in_i == jnp.where(out_i < layers, 2 * out_i, 2 * (out_i - layers) + 1), 1.0, 0.0
    ).astype(half)
    back_x = lax.broadcasted_iota(jnp.int32, (LANE, rest), 0)
    back_t = lax.broadcasted_iota(jnp.int32, (LANE, rest), 1)

    def weigh(s):
        n = s % per_tile
        wts[s, :main, :] = jnp.dot(spec[s, :main, :], perm, preferred_element_type=jnp.float32).astype(half)
        back = jnp.where(back_x == back_t + n * rest, 1.0, 0.0).astype(half)
        tails = jnp.dot(spec[s, main:, :], perm, preferred_element_type=jnp.float32).astype(half)
        wts[s, main:, :] = jnp.dot(back, tails, preferred_element_type=jnp.float32).astype(half)

    fine = lax.broadcasted_iota(jnp.int32, (KB, LANE), 1).astype(jnp.float32)
    lane = lax.broadcasted_iota(jnp.int32, (KB, LANE), 1)
    pieces = kchunk // KB
    steps = rows // ROW_STEP

    def row_count(r):
        a = lat[wi * rows + r]
        return 20 + 4 * jnp.minimum(a, NLAT - 1 - a)

    def basis_rows(c):
        for group, start in zip(groups, group_starts):
            if c in group:
                real = start + group.index(c) * kchunk
                return real, real + len(group) * kchunk

    group_starts = []
    for group in groups:
        group_starts.append(2 * kchunk * sum(len(g) for g in groups[: len(group_starts)]))

    def make_basis(c, unit):
        real0, imag0 = basis_rows(c)
        k0 = unit // steps * KB
        r0 = unit % steps * ROW_STEP
        m = waves[c * kchunk + k0 : c * kchunk + k0 + KB, :]
        counts = [row_count(r0 + i) for i in range(ROW_STEP)]
        each = jnp.full((KB, LANE), counts[0].astype(jnp.float32), jnp.float32)
        for i in range(1, ROW_STEP):
            each = jnp.where(lane == i, counts[i].astype(jnp.float32), each)
        stride_cos, stride_sin = trig(m * LANE, each, 1.0 / each)
        for i in range(ROW_STEP):
            r = r0 + i
            highest = jnp.minimum(wave_count - 1, lax.shift_right_logical(counts[i] - 1, 1)).astype(jnp.float32)
            count = jnp.full((KB, LANE), counts[i].astype(jnp.float32), jnp.float32)
            factor = jnp.where((m >= 0.0) & (m <= highest), jnp.where(m == 0.0, 1.0, 2.0), 0.0)
            sc = jnp.broadcast_to(stride_cos[:, i : i + 1], (KB, LANE))
            ss = jnp.broadcast_to(stride_sin[:, i : i + 1], (KB, LANE))
            c0, s0 = trig(m * fine, count, 1.0 / count)
            c0 = c0 * factor
            s0 = -(s0 * factor)
            c1 = c0 * sc + s0 * ss
            s1 = s0 * sc - c0 * ss
            twice = sc + sc
            final = c in groups[-1]
            table = late if final else basis
            base = group_starts[-1] if final else 0
            for b in range(blocks):
                keep = lane + b * LANE < counts[i]
                cb, sb = (jnp.where(keep, c0, 0.0), jnp.where(keep, s0, 0.0)) if final else (c0, s0)
                table[r, b, real0 - base + k0 : real0 - base + k0 + KB, :] = cb.astype(half)
                table[r, b, imag0 - base + k0 : imag0 - base + k0 + KB, :] = sb.astype(half)
                if b + 1 < blocks:
                    c0, c1 = c1, twice * c1 - c0
                    s0, s1 = s1, twice * s1 - s0

    cols = lax.broadcasted_iota(jnp.int32, (1, main), 1)
    tcols = lax.broadcasted_iota(jnp.int32, (1, LANE), 1)

    def fourier(c):
        lo, hi = bounds[c]
        for s in range(lo, hi):
            border = wave_count - wp[wi * slots + s]
            fold_rows = jnp.concatenate([cols, main + tcols - s % per_tile * rest], axis=1)
            low = jnp.where(fold_rows < border, 1.0, 0.0).astype(half)
            values = jnp.concatenate([
                leg[:, s].reshape(qtot, main),
                tail[:, s // per_tile].reshape(qtot, LANE),
            ], axis=1)
            picked = values * low
            f = jnp.dot(
                jnp.concatenate([picked, values - picked], axis=0), wts[s],
                preferred_element_type=jnp.float32,
            )
            for h in range(HALVES):
                stage[pl.ds(h * PACK + s - lo, qtot, stride=SIDE), :] = f[h * qtot : (h + 1) * qtot]
        snd[c * nw : (c + 1) * nw] = stage[...].astype(half).reshape((nw,) + snd.shape[1:])
        for k in order:
            exchange(c, k).start()
        mine = stage[pl.ds(pl.multiple_of(wi * rows * SIDE, rows * SIDE), rows * SIDE), :]
        rcv[c, wi] = mine.astype(half).reshape(rcv.shape[2:])

    def landed(c):
        others = pl.ds(0, nw - 1)
        exchanged(c, rcv.at[c, others], rcv.at[c, others]).wait_recv()

    lanes = lax.broadcasted_iota(jnp.int32, (layers, COLS), 1)

    def synthesis(g):
        group = groups[g]
        for c in group:
            landed(c)
        depth = 2 * kchunk * len(group)

        def body(r, carry):
            v = jnp.concatenate([rcv[c, :, r].reshape(kchunk, items) for c in group], axis=0)
            vt = v.T
            lhs = jnp.concatenate([vt[:layers], vt[layers:]], axis=1)
            count = row_count(r)
            for n0 in range(0, full, COLS):
                n1 = min(full, n0 + COLS)
                rhs = jnp.concatenate([
                    basis[r, b, group_starts[g] : group_starts[g] + depth, :]
                    for b in range(n0 // LANE, n1 // LANE)
                ], axis=1)
                value = jnp.dot(lhs, rhs, preferred_element_type=jnp.float32)
                if g:
                    value = part[r, :, n0:n1] + value
                if g + 2 == len(groups):
                    value = jnp.where(lanes[:, : n1 - n0] + n0 < count, value, 0.0)
                part[r, :, n0:n1] = value
            return carry

        lax.fori_loop(0, rows, body, 0, unroll=True)

    units = [(c, unit) for c in range(chunks) for unit in range(pieces * steps)]
    pace = -(-slots // len(units))
    done = {"weighed": 0, "made": 0}

    def prepare(upto):
        while done["weighed"] < min(slots, upto):
            weigh(done["weighed"])
            done["weighed"] += 1

    def work(upto):
        while done["made"] < min(len(units), upto):
            prepare(done["weighed"] + pace)
            make_basis(*units[done["made"]])
            done["made"] += 1

    spec_copy.wait()
    polls = sorted(((k, c) for k in range(nl - 1) for c in range(chunks)), key=lambda p: (1.5 * p[0] + p[1], p[0]))
    shown = 0
    for k, c in polls:
        arrive(k, c)
        if k == 0 and ahead < chunks:
            send(0, ahead)
            ahead += 1
        if k == nl - 2:
            prepare(bounds[c][1])
            if c == 0:
                everyone()
            fourier(c)
            while shown < len(groups) and groups[shown][-1] + 3 <= c:
                work(len(units) // chunks * (groups[shown][-1] + 1))
                synthesis(shown)
                shown += 1
        work(done["made"] + 1)
    work(len(units))
    while shown < len(groups) - 1:
        synthesis(shown)
        shown += 1

    for place in range(nl):
        for way, number in ((0, place + 1), (1, nl - place)):
            if number < nl:
                @pl.when(li == place)
                def _():
                    every = pl.ds(0, number)
                    hop(way, 0, leg.at[every], 0, main_recv.at[0, 0]).wait_send()
                    hop(way, 0, tail.at[every], 1, tail_recv.at[0, 0]).wait_send()

    sent = snd.at[pl.ds(0, chunks * (nw - 1))]
    exchanged(0, sent, sent).wait_send()

    for n, c in enumerate(groups[-1]):
        landed(c)
        got[n] = rcv[c]


def finish(alone, part, late, got, out_hbm, rows_buf, out_sem):
    rows, layers, width = out_hbm.shape
    full = part.shape[2]
    items = got.shape[-1]
    depth = got.shape[1] * got.shape[3]
    for r in range(rows):
        v = jnp.concatenate([got[n, :, r].reshape(depth, items) for n in range(got.shape[0])], axis=0)
        vt = v.T
        lhs = jnp.concatenate([vt[:layers], vt[layers:]], axis=1)
        for n0 in range(0, full, COLS):
            n1 = min(full, n0 + COLS)
            rhs = jnp.concatenate([late[r, b] for b in range(n0 // LANE, n1 // LANE)], axis=1)
            value = jnp.dot(lhs, rhs, preferred_element_type=jnp.float32)
            if not alone:
                value = part[r, :, n0:n1] + value
            stop = min(width, n1)
            rows_buf[r, :, n0:stop] = value[:, : stop - n0].astype(jnp.bfloat16)
        pltpu.make_async_copy(rows_buf.at[r], out_hbm.at[r], out_sem.at[r]).start()
    for r in range(rows):
        pltpu.make_async_copy(rows_buf.at[r], out_hbm.at[r], out_sem.at[r]).wait()


def on_device(spectral, legendre, wave_pair, lat_slot):
    slots, fold, items = spectral.shape
    wave_count = fold - 1
    nw = lax.axis_size("wav")
    nl = lax.axis_size("lev")
    rows = lat_slot.shape[0] // nw
    layers = items // 2
    width = 2 * NLAT + 16
    full = -(-width // LANE) * LANE
    main = fold // LANE * LANE
    per_tile = LANE // (fold - main)
    bounds = chunk_plan(slots, per_tile)
    chunks = len(bounds)
    groups = group_plan(chunks)
    tiles = -(-slots // per_tile)
    leg_t = jnp.transpose(legendre, (0, 2, 1))
    lrows = leg_t.shape[1]
    kchunk = nw * SIDE

    bits = (nw >> 1).bit_length() - 1
    stages = max(0, bits - 1) if nw & (nw - 1) == 0 else 0

    hbm = pl.BlockSpec(memory_space=pl.ANY)
    dma = pltpu.SemaphoreType.DMA
    vmem = pltpu.VMEM
    half = jnp.bfloat16
    place = functools.partial(pltpu.with_memory_space_constraint, memory_space=pltpu.HBM)
    last = 2 * kchunk * len(groups[-1])
    handed = pl.pallas_call(
        functools.partial(kernel, nw, nl, slots, wave_count, bounds, groups, per_tile),
        out_shape=[
            vmem((rows, layers, full), jnp.float32),
            vmem((rows, full // LANE, last, LANE), half),
            vmem((len(groups[-1]), nw, rows, SIDE, items), half),
        ],
        in_specs=[hbm, hbm, hbm, hbm],
        out_specs=[pl.BlockSpec(memory_space=vmem)] * 3,
        scratch_shapes=[
            pltpu.SMEM(wave_pair.shape, jnp.int32),
            pltpu.SMEM(lat_slot.shape, jnp.int32),
            vmem((slots, fold, items), half),
            vmem((slots, lrows, fold), half),
            vmem((nl, slots, lrows, main), half),
            vmem((nl, tiles, lrows, LANE), half),
            vmem((slots, main + LANE, items), half),
            vmem((chunks * kchunk, LANE), jnp.float32),
            vmem((nw * rows * SIDE, items), jnp.float32),
            vmem((chunks * nw, rows, SIDE, items), half),
            vmem((chunks, nw, rows, SIDE, items), half),
            vmem((rows, full // LANE, 2 * chunks * kchunk - last, LANE), half),
            dma((5,)),
            dma((2, 2)),
            dma((nl - 1, chunks)),
            dma((nl - 1, tiles)),
            dma((1,)),
            dma((chunks,)),
            pltpu.SemaphoreType.REGULAR((2 + stages,)),
        ],
        compiler_params=pltpu.CompilerParams(collective_id=0, has_side_effects=True, vmem_limit_bytes=44 << 20),
    )(place(wave_pair), place(lat_slot), place(spectral), place(leg_t))
    return pl.pallas_call(
        functools.partial(finish, len(groups) == 1),
        out_shape=jax.ShapeDtypeStruct((rows, layers, width), half),
        in_specs=[pl.BlockSpec(memory_space=vmem)] * 3,
        out_specs=hbm,
        scratch_shapes=[vmem((rows, layers, width), half), dma((rows,))],
        compiler_params=pltpu.CompilerParams(vmem_limit_bytes=8 << 20),
    )(*handed)


def solution(mesh):
    return jax.shard_map(
        on_device,
        mesh=mesh,
        in_specs=(P("wav", None, "lev"), P("wav", None, "lev"), P(), P()),
        out_specs=P("wav", "lev", None),
        check_vma=False,
    )
```
